32 devices in a mesh: field: 2 (over core), dom: 16 (over z, y, x).
Axes of the slice: x: 2, y: 2, z: 4, core: 2. Of those that a mesh axis runs over, the one named last changes fastest.
Arguments:
- modes: float32 [2, 40, 131072], P('field', None, 'dom'), may hold values from -6 to 6
- previous: float32 [2, 40, 131072], P('field', None, 'dom'), may hold values from -6 to 6
- kinds: int32 [2, 3, 256], P('field'), may hold values from 0 to 3
- scales: float32 [2, 3, 256], P('field'), may hold values from 0.5 to 4
- tables: bfloat16 [2, 3, 4, 512, 512], P('field'), may hold values from -2 to 6, as said below
- wet_rows: int32 [2, 49152], P('field', 'dom'), may hold values from 0 to 8191, as said below
- wet_counts: int32 [16], P('dom'), may hold values from 768 to 3072, as said below
- coupling: float32 [49152], P('dom'), may hold values from -6 to 6
Outputs:
- basis: float32 [2, 120, 131072], P('field', None, 'dom')
- projected: float32 [120, 120], replicated
The draws below stay inside these ranges and needn't reach their ends.
Inputs may be any that keep to these rules, and one draw needn't show every extreme that they name: `tables`: tables of offset 0 are symmetric. `wet_rows`: within each subdomain and field the 3072 row numbers are distinct. `wet_counts`: some subdomain uses all 3072 slots.
All inputs are finite; a program needn't handle non-finite values.
Results may differ from the reference program's by a relative error of at most 0.00045.
The reference program's roundings to bfloat16 on the way count: a program that leaves them out, or rounds other values in their place, can miss the bound.
Values may be sent and summed in bfloat16 or wider, within the bound.
A program may use at most 192 MiB of HBM per device.

```python
import math
import jax
import jax.numpy as jnp
from jax import lax

MODES = 40
BS = 512
NTYPE = 4
NBR = 16
ROWS_DEV = 8192
IFACE = 3072
SUBDOMS = 16
NBLK = 256
NF = 131072


def draw_tables(key, part):
    first, second = jax.random.split(key, 2)
    shape = (2, 3, NTYPE, BS, BS)
    noise = jnp.clip(jax.random.normal(first, shape, jnp.float32), -4.0, 4.0)
    noise = noise / jnp.sqrt(jnp.float32(BS))
    symmetric = (noise + jnp.swapaxes(noise, -1, -2)) * 0.70710678
    diagonal = jax.random.uniform(second, (2, 3, NTYPE, BS), jnp.float32, 2.0, 4.0)
    identity = jnp.eye(BS, dtype=jnp.float32)
    centre = symmetric + identity * diagonal[..., None]
    which = jnp.arange(3)[None, :, None, None, None] == 0
    return jnp.where(which, centre, noise).astype(jnp.bfloat16)


def draw_wet_rows(key, part):
    keys = jax.random.split(jax.random.fold_in(key, 11), 2 * SUBDOMS)
    chosen = jax.vmap(lambda single: jax.random.permutation(single, ROWS_DEV)[:IFACE])(keys)
    return chosen.reshape(2, SUBDOMS * IFACE).astype(jnp.int32)


def draw_wet_counts(key, part):
    first, second = jax.random.split(jax.random.fold_in(key, 23), 2)
    counts = jax.random.randint(first, (SUBDOMS,), IFACE // 4, IFACE + 1)
    fullest = jax.random.randint(second, (), 0, SUBDOMS)
    return jnp.where(jnp.arange(SUBDOMS) == fullest, IFACE, counts).astype(jnp.int32)


def place_ends(array, own_key, smallest, high):
    longest = array.shape.index(max(array.shape))
    spots = []
    for shift in (0, 1):
        where = [jax.random.randint(jax.random.fold_in(own_key, axis), (), 0, length) for axis, length in enumerate(array.shape)]
        where[longest] = (where[longest] + shift) % array.shape[longest]
        spots.append(tuple(where))
    return array.at[spots[0]].set(smallest).at[spots[1]].set(high)


def block_scale(own_key, extent, cuts, smallest, top_value):
    def one(position, parts):
        heights = jax.random.uniform(jax.random.fold_in(jax.random.fold_in(own_key, 6), position), (parts,), jnp.float32, smallest / len(cuts), top_value / len(cuts))
        return jnp.repeat(jnp.exp(heights), extent[position] // parts).reshape((-1,) + (1,) * (len(extent) - position - 1))

    factor_of = one(*cuts[0])
    for cut in cuts[1:]:
        factor_of = factor_of * one(*cut)
    return factor_of


def bell_draw(own_key, shape, deviation, limit, cuts=(), kind=jnp.bfloat16):
    values = jax.random.normal(own_key, shape, jnp.float32) * deviation
    if len(cuts) > 0:
        values = block_scale(own_key, shape, cuts, -0.22, 0.18) * values
    return jnp.clip(values, min=-limit, max=limit).astype(kind)


def setup_inputs(seed: int = 0) -> dict:
    splits = jax.random.split(jax.random.key(seed), 9)
    return {
        "modes": bell_draw(splits[0], (2, MODES, NF), 1.0, 6.0, ((0, 2), (2, 16)), jnp.float32),
        "previous": bell_draw(splits[1], (2, MODES, NF), 1.0, 6.0, ((0, 2), (2, 16)), jnp.float32),
        "kinds": place_ends(jax.random.randint(splits[2], (2, 3, NBLK), 0, NTYPE), jax.random.fold_in(splits[2], 1), 0, NTYPE - 1).astype(jnp.int32),
        "scales": jnp.clip(jnp.exp(math.log(4.0) - 2.0794415 * jax.random.uniform(splits[3], (2, 3, NBLK), jnp.float32) ** block_scale(splits[3], (2, 3, NBLK), ((0, 2),), -0.2, 0.2)), 0.5, 4.0),
        "tables": draw_tables(jax.random.fold_in(splits[8], 71), 0),
        "wet_rows": draw_wet_rows(jax.random.fold_in(splits[8], 71), 0),
        "wet_counts": draw_wet_counts(jax.random.fold_in(splits[8], 71), 0),
        "coupling": bell_draw(splits[7], (SUBDOMS * IFACE,), 1.0, 6.0, ((0, 16),), jnp.float32),
    }


def block_product(window, kinds, scales, tables):
    columns = window.shape[0]
    blocks = window.reshape(columns, NBR + 4, BS).astype(jnp.float32)
    centre = tables[0][kinds[0, 2:]].astype(jnp.float32)
    result = scales[0, 2:][None, :, None] * jnp.einsum('cni,nji->cnj', blocks[:, 2:NBR + 2], centre)
    for offset in (1, 2):
        ahead = tables[offset][kinds[offset, 2:]].astype(jnp.float32)
        result = result + scales[offset, 2:][None, :, None] * jnp.einsum('cni,nji->cnj', blocks[:, 2 + offset:NBR + 2 + offset], ahead)
        behind = tables[offset][kinds[offset, 2 - offset:NBR + 2 - offset]].astype(jnp.float32)
        result = result + scales[offset, 2 - offset:NBR + 2 - offset][None, :, None] * jnp.einsum('cni,nij->cnj', blocks[:, 2 - offset:NBR + 2 - offset], behind)
    return result.reshape(columns, NBR * BS)

def field_blocks(vectors, kinds, scales, tables):
    columns = vectors.shape[0]
    padded = jnp.pad(vectors.astype(jnp.bfloat16), ((0, 0), (2 * BS, 2 * BS)))
    kinds_pad = jnp.pad(kinds, ((0, 0), (2, 0)))
    scales_pad = jnp.pad(scales, ((0, 0), (2, 0)))

    def one_domain(domain):
        window = lax.dynamic_slice_in_dim(padded, domain * ROWS_DEV, ROWS_DEV + 4 * BS, 1)
        local_kinds = lax.dynamic_slice_in_dim(kinds_pad, domain * NBR, NBR + 2, 1)
        local_scales = lax.dynamic_slice_in_dim(scales_pad, domain * NBR, NBR + 2, 1)
        return block_product(window, local_kinds, local_scales, tables)
    pieces = lax.map(one_domain, jnp.arange(SUBDOMS, dtype=jnp.int32))
    return jnp.transpose(pieces, (1, 0, 2)).reshape(columns, SUBDOMS * ROWS_DEV)

def operator(vectors, kinds, scales, tables, global_rows, weights):
    images = [field_blocks(vectors[field_id], kinds[field_id], scales[field_id], tables[field_id]) for field_id in range(2)]
    coupled = []
    for field_id in range(2):
        other = 1 - field_id
        values = vectors[other][:, global_rows[other]] * weights[None, :]
        coupled.append(images[field_id].at[:, global_rows[field_id]].add(values))
    return jnp.stack(coupled)

def reference(modes, previous, kinds, scales, tables, wet_rows, wet_counts, coupling):
    highest = lax.Precision.HIGHEST
    offsets = jnp.arange(SUBDOMS, dtype=jnp.int32)[:, None] * ROWS_DEV
    global_rows = (wet_rows.reshape(2, SUBDOMS, IFACE) + offsets[None]).reshape(2, SUBDOMS * IFACE)
    used = jnp.arange(IFACE, dtype=jnp.int32)[None, :] < wet_counts[:, None]
    weights = jnp.where(used, coupling.reshape(SUBDOMS, IFACE), jnp.float32(0.0)).reshape(SUBDOMS * IFACE)
    image_x = operator(modes, kinds, scales, tables, global_rows, weights)
    quotient = jnp.sum(modes * image_x, axis=(0, 2)) / jnp.sum(modes * modes, axis=(0, 2))
    diag_table = jnp.diagonal(tables[:, 0], axis1=-2, axis2=-1).astype(jnp.float32)
    jacobi = jnp.stack([(scales[field_id, 0][:, None] * diag_table[field_id][kinds[field_id, 0]]).reshape(SUBDOMS * ROWS_DEV) for field_id in range(2)])
    residual_dir = (image_x - modes * quotient[None, :, None]) / jacobi[:, None, :]
    image_wp = operator(jnp.concatenate([residual_dir, previous], axis=1), kinds, scales, tables, global_rows, weights)
    search = jnp.concatenate([modes, residual_dir, previous], axis=1)
    image_all = jnp.concatenate([image_x, image_wp], axis=1)
    ndof = 2.0 * SUBDOMS * ROWS_DEV
    gram_b = (jnp.dot(search[0], search[0].T, precision=highest) + jnp.dot(search[1], search[1].T, precision=highest)) / ndof
    raw = jnp.dot(search[0], image_all[0].T, precision=highest) + jnp.dot(search[1], image_all[1].T, precision=highest)
    gram_a = (raw + raw.T) / (2.0 * ndof)
    chol = jnp.linalg.cholesky(gram_b)
    leading = jax.scipy.linalg.solve_triangular(chol, gram_a, lower=True)
    projected = jax.scipy.linalg.solve_triangular(chol, leading.T, lower=True)
    basis = jnp.stack([jax.scipy.linalg.solve_triangular(chol, search[field_id], lower=True) for field_id in range(2)])
    return (basis, projected)
```

```python
import functools

import jax
import jax.numpy as jnp
from jax import lax
from jax.experimental import pallas as pl
from jax.experimental.pallas import tpu as pltpu
from jax.sharding import PartitionSpec as P

BS = 512
LANES = 128
SHIFT = 16


def swapped(shard, axis, apart):
    return lax.ppermute(shard, axis, [(i, i ^ 1 << apart) for i in range(lax.axis_size(axis))])


def halos(cells, axis, dim, width):
    count = lax.axis_size(axis)
    ends = count - 1
    head = lax.slice_in_dim(cells, 0, width, axis=dim)
    tail = lax.slice_in_dim(cells, cells.shape[dim] - width, cells.shape[dim], axis=dim)
    return (
        lax.ppermute(tail, axis, [(i, i + 1) for i in range(ends)]),
        lax.ppermute(head, axis, [(i + 1, i) for i in range(ends)]),
    )


def sum_kernel(rounds, split, x_ref, o_ref, held, landed, across, send_sem, recv_sem, side_send, side_recv):
    field = lax.axis_index("field")
    dom = lax.axis_index("dom")
    groups = []
    for step, members in rounds:
        low = (1 - 2 * ((dom // step) % 2)) * step
        high = (1 - 2 * ((dom // (2 * step)) % 2)) * 2 * step
        groups.append([dom + (e % 2) * low + (e // 2) * high for e in range(1, members)])
    barrier = pltpu.get_barrier_semaphore()
    peers = [(1 - field, dom)] + [(field, peer) for group in groups for peer in group]
    for peer in peers:
        pl.semaphore_signal(barrier, inc=1, device_id=peer, device_id_type=pl.DeviceIdType.MESH)
    pl.semaphore_wait(barrier, len(peers))

    def send(source, target, sems, peer):
        copy = pltpu.make_async_remote_copy(
            src_ref=source,
            dst_ref=target,
            send_sem=sems[0],
            recv_sem=sems[1],
            device_id=peer,
            device_id_type=pl.DeviceIdType.MESH,
        )
        copy.start()
        return copy

    mine, theirs = (field, 1 - field) if split else (0, 0)
    copy = send(
        x_ref.at[theirs], across.at[0], (side_send.at[0], side_recv.at[0]), (1 - field, dom)
    )
    copy.wait()
    total = x_ref[mine] + across[0]
    for turn, group in enumerate(groups):
        held[turn] = total
        copies = [
            send(
                held.at[turn],
                landed.at[turn, e],
                (send_sem.at[turn, e], recv_sem.at[turn, e]),
                (field, peer),
            )
            for e, peer in enumerate(group)
        ]
        for copy in copies:
            copy.wait()
        total = total + landed[turn, 0]
        if len(group) == 3:
            total = total + (landed[turn, 1] + landed[turn, 2])
    o_ref[mine] = total
    if split:
        held[len(groups)] = total
        copy = send(
            held.at[len(groups)],
            across.at[1],
            (side_send.at[1], side_recv.at[1]),
            (1 - field, dom),
        )
        copy.wait()
        o_ref[theirs] = across[1]


def summed_everywhere(x, collective_id):
    bits = (lax.axis_size("dom") - 1).bit_length()
    rounds = [(1 << bit, 4 if bit + 1 < bits else 2) for bit in range(0, bits, 2)]
    cell = x.shape[1:]
    slots = len(rounds)
    return pl.pallas_call(
        functools.partial(sum_kernel, rounds, x.shape[0] == 2),
        out_shape=jax.ShapeDtypeStruct(x.shape, x.dtype),
        in_specs=[pl.BlockSpec(memory_space=pltpu.VMEM)],
        out_specs=pl.BlockSpec(memory_space=pltpu.VMEM),
        scratch_shapes=[
            pltpu.VMEM((slots + 1,) + cell, x.dtype),
            pltpu.VMEM((slots, 3) + cell, x.dtype),
            pltpu.VMEM((2,) + cell, x.dtype),
            pltpu.SemaphoreType.DMA((slots, 3)),
            pltpu.SemaphoreType.DMA((slots, 3)),
            pltpu.SemaphoreType.DMA((2,)),
            pltpu.SemaphoreType.DMA((2,)),
        ],
        compiler_params=pltpu.CompilerParams(
            collective_id=collective_id, has_side_effects=True
        ),
    )(x)


NN = (((1,), (0,)), ((), ()))
NT = (((1,), (1,)), ((), ()))


def operator_kernel(
    kinds, scales, places, weights, x_ref, before, after, other, tables, o_ref, window, rows_in, rows_out
):
    columns, wide = x_ref.shape
    nbr = wide // BS
    share = places.shape[0] // nbr
    window[:, : 2 * BS] = before[...]
    window[:, 2 * BS : 2 * BS + wide] = x_ref[...].astype(jnp.bfloat16)
    window[:, 2 * BS + wide :] = after[...]
    blank = jnp.zeros((LANES - columns, LANES), jnp.float32)

    def turn_in(tile, carry):
        span = pl.ds(pl.multiple_of(tile * LANES, LANES), LANES)
        cell = jnp.concatenate([other[:, span].astype(jnp.float32), blank], axis=0)
        rows_in[span, :] = cell.T
        rows_out[span, :] = jnp.zeros((LANES, LANES), jnp.float32)
        return carry

    lax.fori_loop(0, wide // LANES, turn_in, 0, unroll=16)

    def term(n, shift, offset, at, dims):
        block = window[:, pl.ds(pl.multiple_of((n + 2 + shift) * BS, BS), BS)]
        product = lax.dot_general(
            block, tables[offset, kinds[offset, at]], dims, preferred_element_type=jnp.float32
        )
        return scales[offset, at] * product

    def step(n, carry):
        total = term(n, 0, 0, n + 2, NN)
        for offset in (1, 2):
            total = total + term(n, offset, offset, n + 2, NT)
            total = total + term(n, -offset, offset, n + 2 - offset, NN)
        o_ref[:, pl.ds(pl.multiple_of(n * BS, BS), BS)] = total
        for slot in range(share):
            place = places[n * share + slot]
            source = lax.shift_right_logical(place, SHIFT)
            target = lax.bitwise_and(place, (1 << SHIFT) - 1)
            rows_out[pl.ds(target, 1), :] = rows_in[pl.ds(source, 1), :] * weights[n * share + slot]
        return carry

    lax.fori_loop(0, nbr, step, 0)

    def turn_out(tile, carry):
        span = pl.ds(pl.multiple_of(tile * LANES, LANES), LANES)
        o_ref[:, span] = o_ref[:, span] + rows_out[span, :].T[:columns]
        return carry

    lax.fori_loop(0, wide // LANES, turn_out, 0, unroll=16)


def operate(vectors, kinds, scales, tables, places, weights):
    columns, wide = vectors.shape
    rounded = vectors.astype(jnp.bfloat16)
    other = swapped(rounded, "field", 0)
    before, after = halos(rounded, "dom", 1, 2 * BS)
    smem = pl.BlockSpec(memory_space=pltpu.SMEM)
    vmem = pl.BlockSpec(memory_space=pltpu.VMEM)
    return pl.pallas_call(
        operator_kernel,
        out_shape=jax.ShapeDtypeStruct((columns, wide), jnp.float32),
        in_specs=[smem, smem, smem, smem, vmem, vmem, vmem, vmem, vmem],
        out_specs=vmem,
        scratch_shapes=[
            pltpu.VMEM((columns, wide + 4 * BS), jnp.bfloat16),
            pltpu.VMEM((wide, LANES), jnp.float32),
            pltpu.VMEM((wide, LANES), jnp.float32),
        ],
        cost_estimate=pl.CostEstimate(
            flops=10 * columns * wide * BS, bytes_accessed=16 * columns * wide, transcendentals=0
        ),
        compiler_params=pltpu.CompilerParams(vmem_limit_bytes=40 * 1024 * 1024),
    )(kinds, scales, places, weights, vectors, before, after, other, tables)


SUB = 8


def split_dot(left, right, dims):
    lh = left.astype(jnp.bfloat16)
    ll = (left - lh.astype(jnp.float32)).astype(jnp.bfloat16)
    rh = right.astype(jnp.bfloat16)
    rl = (right - rh.astype(jnp.float32)).astype(jnp.bfloat16)

    def dot(a, b):
        return lax.dot_general(a, b, dims, preferred_element_type=jnp.float32)

    return dot(lh, rh) + (dot(lh, rl) + dot(ll, rh))


def eliminate(gram, size, inverse_ref):
    panels = size // SUB
    sub = lax.broadcasted_iota(jnp.int32, (SUB, LANES), 0)
    lane = lax.broadcasted_iota(jnp.int32, (SUB, LANES), 1)
    left = [gram[SUB * i : SUB * (i + 1)] for i in range(panels)]
    right = [(lane == sub + SUB * i).astype(jnp.float32) for i in range(panels)]

    def over_lanes(cell, column):
        return jnp.broadcast_to(cell[:, column : column + 1], (SUB, LANES))

    def over_rows(cell, row):
        return jnp.broadcast_to(cell[row : row + 1], (SUB, LANES))

    for k in range(panels):
        columns = [over_lanes(left[k], SUB * k + c) for c in range(SUB)]
        cells = [left[k], right[k]]
        for c in range(SUB):
            pivot = over_rows(columns[c], c)
            inverse = 1.0 / pivot
            inverse_ref[SUB * k + c : SUB * k + c + 1] = (cells[1] * lax.rsqrt(pivot))[c : c + 1]
            here = sub == c
            factor = columns[c]

            def reduced(cell):
                row = over_rows(cell, c) * inverse
                return jnp.where(here, row, cell - factor * row)

            for later in range(c + 1, SUB):
                columns[later] = reduced(columns[later])
            cells = [reduced(cell) for cell in cells]
        rows = [[over_rows(cell, c) for c in range(SUB)] for cell in cells]
        for i in range(k + 1, panels):
            source = left[i]
            for c in range(SUB):
                factor = over_lanes(source, SUB * k + c)
                left[i] = left[i] - factor * rows[0][c]
                right[i] = right[i] - factor * rows[1][c]


def finish_kernel(chunk, scale, packed_ref, x_ref, r_ref, p_ref, basis_ref, projected_ref, inverse_ref, held, sems):
    columns, wide = x_ref.shape
    size = 3 * columns
    packed = packed_ref[...] * scale
    row = lax.broadcasted_iota(jnp.int32, packed.shape, 0)
    col = lax.broadcasted_iota(jnp.int32, packed.shape, 1)
    gram_b = jnp.where(col <= row, packed, packed.T)
    inverse_ref[...] = jnp.zeros_like(inverse_ref)
    eliminate(gram_b, size, inverse_ref)
    high = jnp.concatenate([packed[:, 1:], packed[:, :1]], axis=1)
    gram_a = jnp.where(col >= row, high, high.T)
    gram_a = jnp.where(jnp.maximum(row, col) < size, 0.5 * gram_a, 0.0)
    inverse = inverse_ref[...]
    projected = split_dot(split_dot(inverse, gram_a, NN), inverse, NT)
    projected_ref[...] = projected[:size, :size]
    ih = inverse.astype(jnp.bfloat16)
    il = (inverse - ih.astype(jnp.float32)).astype(jnp.bfloat16)
    twice = jnp.concatenate([ih, ih], axis=1)
    blank = jnp.zeros((LANES - size, chunk), jnp.float32)

    def copy(n):
        span = pl.ds(pl.multiple_of(n * chunk, chunk), chunk)
        return pltpu.make_async_copy(held.at[n], basis_ref.at[0, :, span], sems.at[n])

    def step(n, carry):
        span = pl.ds(pl.multiple_of(n * chunk, chunk), chunk)
        search = jnp.concatenate([x_ref[:, span], r_ref[:, span], p_ref[:, span], blank], axis=0)
        sh = search.astype(jnp.bfloat16)
        sl = (search - sh.astype(jnp.float32)).astype(jnp.bfloat16)
        both = jnp.concatenate([sh, sl], axis=0)
        out = lax.dot_general(twice, both, NN, preferred_element_type=jnp.float32)
        out = out + lax.dot_general(il, sh, NN, preferred_element_type=jnp.float32)
        held[n] = out[:size]
        copy(n).start()
        return carry

    lax.fori_loop(0, wide // chunk, step, 0)

    def close(n, carry):
        copy(n).wait()
        return carry

    lax.fori_loop(0, wide // chunk, close, 0)


def finish(packed, vec_modes, residual_dir, vec_prev, ndof):
    columns, wide = vec_modes.shape
    size = 3 * columns
    chunk = min(512, wide)
    vmem = pl.BlockSpec(memory_space=pltpu.VMEM)
    return pl.pallas_call(
        functools.partial(finish_kernel, chunk, 1.0 / ndof),
        out_shape=(
            jax.ShapeDtypeStruct((1, size, wide), jnp.float32),
            jax.ShapeDtypeStruct((size, size), jnp.float32),
        ),
        in_specs=[vmem, vmem, vmem, vmem],
        out_specs=(pl.BlockSpec(memory_space=pl.ANY), vmem),
        scratch_shapes=[
            pltpu.VMEM((LANES, LANES), jnp.float32),
            pltpu.VMEM((wide // chunk, size, chunk), jnp.float32),
            pltpu.SemaphoreType.DMA((wide // chunk,)),
        ],
        cost_estimate=pl.CostEstimate(
            flops=6 * size * size * wide, bytes_accessed=8 * size * wide, transcendentals=0
        ),
        compiler_params=pltpu.CompilerParams(vmem_limit_bytes=24 * 1024 * 1024),
    )(packed, vec_modes, residual_dir, vec_prev)


def shards(modes, previous, kinds, scales, tables, wet_rows, wet_counts, coupling):
    high = lax.Precision.HIGH
    domain = lax.axis_index("dom")
    vec_modes = modes[0]
    vec_prev = previous[0]
    columns, wide = vec_modes.shape
    nbr = wide // BS
    field_tables = tables[0]
    types = field_tables.shape[1]
    kinds_pad = jnp.pad(kinds[0], ((0, 0), (2, 0)))
    scales_pad = jnp.pad(scales[0], ((0, 0), (2, 0)))
    local_kinds = lax.dynamic_slice_in_dim(kinds_pad, domain * nbr, nbr + 2, 1)
    local_scales = lax.dynamic_slice_in_dim(scales_pad, domain * nbr, nbr + 2, 1)
    rows = wet_rows[0]
    slots = coupling.shape[0]
    used = jnp.arange(slots, dtype=jnp.int32) < wet_counts[0]
    weights = jnp.where(used, coupling, jnp.float32(0.0))
    places = (swapped(rows, "field", 0) << SHIFT) | rows
    operands = (local_kinds, local_scales, field_tables, places, weights)
    first_pair = jnp.concatenate([vec_modes, vec_prev], axis=0)
    image_pair = operate(first_pair, *operands)
    image_x, image_p = image_pair[:columns], image_pair[columns:]
    partial_sums = jnp.stack(
        [jnp.sum(vec_modes * vec_modes, axis=1), jnp.sum(vec_modes * image_x, axis=1)]
    )
    sums = summed_everywhere(jnp.pad(partial_sums, ((0, 6), (0, LANES - columns)))[None], 1)[0]
    quotient = sums[1, :columns] / sums[0, :columns]
    eye = jnp.eye(BS, dtype=jnp.bool_)
    diag_table = jnp.sum(
        jnp.where(eye[None], field_tables[0].astype(jnp.float32), jnp.float32(0.0)), axis=1
    )
    row_diag = jnp.zeros((nbr, BS), jnp.float32)
    for type_id in range(types):
        row_diag = jnp.where(
            (local_kinds[0, 2:] == type_id)[:, None], diag_table[type_id][None, :], row_diag
        )
    jacobi = (local_scales[0, 2:][:, None] * row_diag).reshape(wide)
    residual_dir = (image_x - vec_modes * quotient[:, None]) / jacobi[None, :]
    image_r = operate(residual_dir, *operands)
    search = jnp.concatenate([vec_modes, residual_dir, vec_prev], axis=0)
    image_all = jnp.concatenate([image_x, image_r, image_p], axis=0)
    ndof = 2.0 * lax.axis_size("dom") * wide
    part_b = jnp.dot(search, search.T, precision=high)
    part_a = jnp.dot(search, image_all.T, precision=high)
    part_a = part_a + part_a.T
    size = 3 * columns
    row = lax.broadcasted_iota(jnp.int32, (size, size + 8), 0)
    col = lax.broadcasted_iota(jnp.int32, (size, size + 8), 1)
    packed = jnp.where(
        col <= row,
        jnp.pad(part_b, ((0, 0), (0, 8))),
        jnp.pad(part_a, ((0, 0), (1, 7))),
    )
    half = -(-size // 16) * 8
    packed = jnp.pad(packed, ((0, 2 * half - size), (0, 0))).reshape(2, half, size + 8)
    packed = summed_everywhere(packed, 2).reshape(2 * half, size + 8)
    return finish(packed, vec_modes, residual_dir, vec_prev, ndof)


def solution(mesh):
    return jax.shard_map(
        shards,
        mesh=mesh,
        in_specs=(
            P("field", None, "dom"),
            P("field", None, "dom"),
            P("field", None, None),
            P("field", None, None),
            P("field", None, None, None, None),
            P("field", "dom"),
            P("dom"),
            P("dom"),
        ),
        out_specs=(P("field", None, "dom"), P()),
        check_vma=False,
    )
```

```python
import functools

import jax
import jax.numpy as jnp
from jax import lax
from jax.experimental import pallas as pl
from jax.experimental.pallas import tpu as pltpu
from jax.sharding import PartitionSpec as P

BS = 512
LANES = 128
GROUP = 4
UNROLL = 64
MESH = pl.DeviceIdType.MESH
NN = (((1,), (0,)), ((), ()))
NT = (((1,), (1,)), ((), ()))


def sum_kernel(rounds, split, x_ref, o_ref, held, landed, across, send_sem, recv_sem, side_send, side_recv):
    field = lax.axis_index("field")
    dom = lax.axis_index("dom")
    groups = []
    for step, members in rounds:
        low = (1 - 2 * ((dom // step) % 2)) * step
        high = (1 - 2 * ((dom // (2 * step)) % 2)) * 2 * step
        groups.append([dom + (e % 2) * low + (e // 2) * high for e in range(1, members)])
    barrier = pltpu.get_barrier_semaphore()
    peers = [(1 - field, dom)] + [(field, peer) for group in groups for peer in group]
    for peer in peers:
        pl.semaphore_signal(barrier, inc=1, device_id=peer, device_id_type=pl.DeviceIdType.MESH)
    pl.semaphore_wait(barrier, len(peers))

    def send(source, target, sems, peer):
        copy = pltpu.make_async_remote_copy(
            src_ref=source,
            dst_ref=target,
            send_sem=sems[0],
            recv_sem=sems[1],
            device_id=peer,
            device_id_type=pl.DeviceIdType.MESH,
        )
        copy.start()
        return copy

    mine, theirs = (field, 1 - field) if split else (0, 0)
    copy = send(
        x_ref.at[theirs], across.at[0], (side_send.at[0], side_recv.at[0]), (1 - field, dom)
    )
    copy.wait()
    total = x_ref[mine] + across[0]
    for turn, group in enumerate(groups):
        held[turn] = total
        copies = [
            send(
                held.at[turn],
                landed.at[turn, e],
                (send_sem.at[turn, e], recv_sem.at[turn, e]),
                (field, peer),
            )
            for e, peer in enumerate(group)
        ]
        for copy in copies:
            copy.wait()
        total = total + landed[turn, 0]
        if len(group) == 3:
            total = total + (landed[turn, 1] + landed[turn, 2])
    o_ref[mine] = total
    if split:
        held[len(groups)] = total
        copy = send(
            held.at[len(groups)],
            across.at[1],
            (side_send.at[1], side_recv.at[1]),
            (1 - field, dom),
        )
        copy.wait()
        o_ref[theirs] = across[1]


def summed_everywhere(x, collective_id):
    bits = (lax.axis_size("dom") - 1).bit_length()
    rounds = [(1 << bit, 4 if bit + 1 < bits else 2) for bit in range(0, bits, 2)]
    cell = x.shape[1:]
    slots = len(rounds)
    return pl.pallas_call(
        functools.partial(sum_kernel, rounds, x.shape[0] == 2),
        out_shape=jax.ShapeDtypeStruct(x.shape, x.dtype),
        in_specs=[pl.BlockSpec(memory_space=pltpu.VMEM)],
        out_specs=pl.BlockSpec(memory_space=pltpu.VMEM),
        scratch_shapes=[
            pltpu.VMEM((slots + 1,) + cell, x.dtype),
            pltpu.VMEM((slots, 3) + cell, x.dtype),
            pltpu.VMEM((2,) + cell, x.dtype),
            pltpu.SemaphoreType.DMA((slots, 3)),
            pltpu.SemaphoreType.DMA((slots, 3)),
            pltpu.SemaphoreType.DMA((2,)),
            pltpu.SemaphoreType.DMA((2,)),
        ],
        compiler_params=pltpu.CompilerParams(
            collective_id=collective_id, has_side_effects=True
        ),
    )(x)


SUB = 8


def split_dot(left, right, dims):
    lh = left.astype(jnp.bfloat16)
    ll = (left - lh.astype(jnp.float32)).astype(jnp.bfloat16)
    rh = right.astype(jnp.bfloat16)
    rl = (right - rh.astype(jnp.float32)).astype(jnp.bfloat16)

    def dot(a, b):
        return lax.dot_general(a, b, dims, preferred_element_type=jnp.float32)

    return dot(lh, rh) + (dot(lh, rl) + dot(ll, rh))


def eliminate(gram, size, inverse_ref):
    panels = size // SUB
    sub = lax.broadcasted_iota(jnp.int32, (SUB, LANES), 0)
    lane = lax.broadcasted_iota(jnp.int32, (SUB, LANES), 1)
    left = [gram[SUB * i : SUB * (i + 1)] for i in range(panels)]
    right = [(lane == sub + SUB * i).astype(jnp.float32) for i in range(panels)]

    def over_lanes(cell, column):
        return jnp.broadcast_to(cell[:, column : column + 1], (SUB, LANES))

    def over_rows(cell, row):
        return jnp.broadcast_to(cell[row : row + 1], (SUB, LANES))

    for k in range(panels):
        columns = [over_lanes(left[k], SUB * k + c) for c in range(SUB)]
        cells = [left[k], right[k]]
        for c in range(SUB):
            pivot = over_rows(columns[c], c)
            inverse = 1.0 / pivot
            inverse_ref[SUB * k + c : SUB * k + c + 1] = (cells[1] * lax.rsqrt(pivot))[c : c + 1]
            here = sub == c
            factor = columns[c]

            def reduced(cell):
                row = over_rows(cell, c) * inverse
                return jnp.where(here, row, cell - factor * row)

            for later in range(c + 1, SUB):
                columns[later] = reduced(columns[later])
            cells = [reduced(cell) for cell in cells]
        rows = [[over_rows(cell, c) for c in range(SUB)] for cell in cells]
        for i in range(k + 1, panels):
            source = left[i]
            for c in range(SUB):
                factor = over_lanes(source, SUB * k + c)
                left[i] = left[i] - factor * rows[0][c]
                right[i] = right[i] - factor * rows[1][c]


def finish_kernel(chunk, scale, packed_ref, x_ref, r_ref, p_ref, basis_ref, projected_ref, inverse_ref, held, sems):
    columns, wide = x_ref.shape
    size = 3 * columns
    packed = packed_ref[...] * scale
    row = lax.broadcasted_iota(jnp.int32, packed.shape, 0)
    col = lax.broadcasted_iota(jnp.int32, packed.shape, 1)
    gram_b = jnp.where(col <= row, packed, packed.T)
    inverse_ref[...] = jnp.zeros_like(inverse_ref)
    eliminate(gram_b, size, inverse_ref)
    high = jnp.concatenate([packed[:, 1:], packed[:, :1]], axis=1)
    gram_a = jnp.where(col >= row, high, high.T)
    gram_a = jnp.where(jnp.maximum(row, col) < size, 0.5 * gram_a, 0.0)
    inverse = inverse_ref[...]
    projected = split_dot(split_dot(inverse, gram_a, NN), inverse, NT)
    projected_ref[...] = projected[:size, :size]
    ih = inverse.astype(jnp.bfloat16)
    il = (inverse - ih.astype(jnp.float32)).astype(jnp.bfloat16)
    twice = jnp.concatenate([ih, ih], axis=1)
    blank = jnp.zeros((LANES - size, chunk), jnp.float32)

    def copy(n):
        span = pl.ds(pl.multiple_of(n * chunk, chunk), chunk)
        return pltpu.make_async_copy(held.at[n], basis_ref.at[0, :, span], sems.at[n])

    def step(n, carry):
        span = pl.ds(pl.multiple_of(n * chunk, chunk), chunk)
        search = jnp.concatenate([x_ref[:, span], r_ref[:, span], p_ref[:, span], blank], axis=0)
        sh = search.astype(jnp.bfloat16)
        sl = (search - sh.astype(jnp.float32)).astype(jnp.bfloat16)
        both = jnp.concatenate([sh, sl], axis=0)
        out = lax.dot_general(twice, both, NN, preferred_element_type=jnp.float32)
        out = out + lax.dot_general(il, sh, NN, preferred_element_type=jnp.float32)
        held[n] = out[:size]
        copy(n).start()
        return carry

    lax.fori_loop(0, wide // chunk, step, 0)

    def close(n, carry):
        copy(n).wait()
        return carry

    lax.fori_loop(0, wide // chunk, close, 0)


def finish(packed, vec_modes, residual_dir, vec_prev, ndof):
    columns, wide = vec_modes.shape
    size = 3 * columns
    chunk = min(512, wide)
    vmem = pl.BlockSpec(memory_space=pltpu.VMEM)
    return pl.pallas_call(
        functools.partial(finish_kernel, chunk, 1.0 / ndof),
        out_shape=(
            jax.ShapeDtypeStruct((1, size, wide), jnp.float32),
            jax.ShapeDtypeStruct((size, size), jnp.float32),
        ),
        in_specs=[vmem, vmem, vmem, vmem],
        out_specs=(pl.BlockSpec(memory_space=pl.ANY), vmem),
        scratch_shapes=[
            pltpu.VMEM((LANES, LANES), jnp.float32),
            pltpu.VMEM((wide // chunk, size, chunk), jnp.float32),
            pltpu.SemaphoreType.DMA((wide // chunk,)),
        ],
        cost_estimate=pl.CostEstimate(
            flops=6 * size * size * wide, bytes_accessed=8 * size * wide, transcendentals=0
        ),
        compiler_params=pltpu.CompilerParams(vmem_limit_bytes=24 * 1024 * 1024),
    )(packed, vec_modes, residual_dir, vec_prev)


def remote(source, target, sems, peer):
    return pltpu.make_async_remote_copy(
        src_ref=source,
        dst_ref=target,
        send_sem=sems[0],
        recv_sem=sems[1],
        device_id=peer,
        device_id_type=MESH,
    )


def greet(peers):
    barrier = pltpu.get_barrier_semaphore()
    for peer in peers:
        pl.semaphore_signal(barrier, inc=1, device_id=peer, device_id_type=MESH)


def greet_ends(field, dom, ends):
    barrier = pltpu.get_barrier_semaphore()

    @pl.when(dom > 0)
    def _():
        pl.semaphore_signal(barrier, inc=1, device_id=(field, dom - 1), device_id_type=MESH)

    @pl.when(dom < ends)
    def _():
        pl.semaphore_signal(barrier, inc=1, device_id=(field, dom + 1), device_id_type=MESH)


def meet(dom, ends, count):
    left = (dom + ends - 1) // ends
    right = (2 * ends - dom - 1) // ends
    pl.semaphore_wait(pltpu.get_barrier_semaphore(), count + left + right)


def clear_ends(window, nbr):
    empty = jnp.zeros((2,) + window.shape[1:], window.dtype)
    window[:2] = empty
    window[nbr + 2 : nbr + 4] = empty


def halo_copies(window, nbr, sems, field, dom):
    send, recv = sems
    left = remote(
        window.at[pl.ds(2, 2)], window.at[pl.ds(nbr + 2, 2)], (send.at[0], recv.at[0]), (field, dom - 1)
    )
    right = remote(
        window.at[pl.ds(nbr, 2)], window.at[pl.ds(0, 2)], (send.at[1], recv.at[1]), (field, dom + 1)
    )
    return left, right


def start_halos(copies, dom, ends):
    left, right = copies

    @pl.when(dom > 0)
    def _():
        left.start()

    @pl.when(dom < ends)
    def _():
        right.start()


def finish_halos(copies, dom, ends):
    left, right = copies

    @pl.when(dom > 0)
    def _():
        left.wait_send()
        right.wait_recv()

    @pl.when(dom < ends)
    def _():
        right.wait_send()
        left.wait_recv()


def send_wet(read, columns, wide, rows, count, coupling, rows_in, picked, outgoing, wet, sems, peer):
    slots = picked.shape[0]
    blank = jnp.zeros((LANES - columns, LANES), jnp.float32)

    def turn_in(tile, carry):
        span = pl.ds(pl.multiple_of(tile * LANES, LANES), LANES)
        rows_in[span, :] = jnp.concatenate([read(span), blank], axis=0).T
        return carry

    lax.fori_loop(0, wide // LANES, turn_in, 0, unroll=16)

    def gather(i, carry):
        for slot in range(UNROLL):
            at = i * UNROLL + slot
            picked[pl.ds(at, 1), :] = rows_in[pl.ds(rows[0, at], 1), :]
        return carry

    lax.fori_loop(0, slots // UNROLL, gather, 0)

    def weigh(i, carry):
        span = pl.ds(pl.multiple_of(i * LANES, LANES), LANES)
        used = i * LANES + lax.broadcasted_iota(jnp.int32, (1, LANES), 1) < count
        weights = jnp.where(used, coupling[pl.ds(i, 1), :], 0.0)
        spread = jnp.broadcast_to(weights, (LANES, LANES)).T
        outgoing[span, :] = (picked[span, :] * spread).astype(jnp.bfloat16)
        return carry

    lax.fori_loop(0, slots // LANES, weigh, 0, unroll=4)
    copy = remote(outgoing, wet, (sems[0].at[0], sems[1].at[0]), peer)
    copy.start()
    return copy


def first_kernel(
    rows, counts, coupling, x_ref, p_ref, window, wet, rows_in, picked, outgoing, side_send, side_recv, end_send, end_recv
):
    field = lax.axis_index("field")
    dom = lax.axis_index("dom")
    ends = lax.axis_size("dom") - 1
    columns, wide = x_ref.shape
    nbr = wide // BS
    clear_ends(window, nbr)
    greet([(1 - field, dom)])
    greet_ends(field, dom, ends)

    def read(span):
        return jnp.concatenate([x_ref[:, span], p_ref[:, span]], axis=0)

    def fill(n, carry):
        span = pl.ds(pl.multiple_of(n * BS, BS), BS)
        window[n + 2] = read(span).astype(jnp.bfloat16)
        return carry

    lax.fori_loop(0, nbr, fill, 0, unroll=2)
    meet(dom, ends, 1)
    halos = halo_copies(window, nbr, (end_send, end_recv), field, dom)
    start_halos(halos, dom, ends)
    copy = send_wet(
        read, 2 * columns, wide, rows, counts[0], coupling, rows_in, picked, outgoing, wet,
        (side_send, side_recv), (1 - field, dom),
    )
    finish_halos(halos, dom, ends)
    copy.wait()


def exchange_scratch(wide, slots):
    return [
        pltpu.VMEM((wide, LANES), jnp.float32),
        pltpu.VMEM((slots, LANES), jnp.float32),
        pltpu.VMEM((slots, LANES), jnp.bfloat16),
        pltpu.SemaphoreType.DMA((1,)),
        pltpu.SemaphoreType.DMA((1,)),
        pltpu.SemaphoreType.DMA((2,)),
        pltpu.SemaphoreType.DMA((2,)),
    ]


def rows_deep(columns):
    return -(-columns // 16) * 16


SMEM = pl.BlockSpec(memory_space=pltpu.SMEM)
VMEM = pl.BlockSpec(memory_space=pltpu.VMEM)


def exchange_first(vec_modes, vec_prev, wet_rows, wet_counts, coupling):
    columns, wide = vec_modes.shape
    slots = wet_rows.shape[1]
    return pl.pallas_call(
        first_kernel,
        out_shape=(
            jax.ShapeDtypeStruct((wide // BS + 5, rows_deep(2 * columns), BS), jnp.bfloat16),
            jax.ShapeDtypeStruct((slots, LANES), jnp.bfloat16),
        ),
        in_specs=[SMEM, SMEM, VMEM, VMEM, VMEM],
        out_specs=(VMEM, VMEM),
        scratch_shapes=exchange_scratch(wide, slots),
        compiler_params=pltpu.CompilerParams(
            collective_id=1, has_side_effects=True, vmem_limit_bytes=32 * 1024 * 1024
        ),
    )(wet_rows, wet_counts, coupling, vec_modes, vec_prev)


def second_kernel(
    rounds, rows, counts, coupling, x_ref, image, jacobi, window, wet, r_ref,
    rows_in, picked, outgoing, side_send, side_recv, end_send, end_recv, held, landed, sum_send, sum_recv,
):
    field = lax.axis_index("field")
    dom = lax.axis_index("dom")
    ends = lax.axis_size("dom") - 1
    columns, wide = x_ref.shape
    nbr = wide // BS
    deep = window.shape[1]
    groups = []
    for turn, (step, members) in enumerate(rounds):
        low = (1 - 2 * ((dom // step) % 2)) * step
        high = (1 - 2 * ((dom // (2 * step)) % 2)) * 2 * step
        group = [(field, dom + (e % 2) * low + (e // 2) * high) for e in range(members)]
        across = [(1 - field, there) for _, there in group] if turn == 0 else []
        groups.append(group[1:] + across)
    clear_ends(window, nbr)
    peers = [peer for group in groups for peer in group]
    greet(peers)
    greet_ends(field, dom, ends)

    def add(n, carry):
        span = pl.ds(pl.multiple_of(n * LANES, LANES), LANES)
        x = x_ref[:, span]
        return carry[0] + x * x, carry[1] + x * image[:columns, span]

    zero = jnp.zeros((columns, LANES), jnp.float32)
    squares, products = lax.fori_loop(0, wide // LANES, add, (zero, zero), unroll=8)
    lane = lax.broadcasted_iota(jnp.int32, (columns, LANES), 1)
    total = jnp.where(
        lane == 0,
        jnp.sum(squares, axis=1, keepdims=True),
        jnp.where(lane == 1, jnp.sum(products, axis=1, keepdims=True), 0.0),
    )
    meet(dom, ends, len(peers))
    for turn, group in enumerate(groups):
        held[turn] = total
        copies = [
            remote(held.at[turn], landed.at[turn, e], (sum_send.at[turn, e], sum_recv.at[turn, e]), peer)
            for e, peer in enumerate(group)
        ]
        for copy in copies:
            copy.start()
        for copy in copies:
            copy.wait()

        def four(parts):
            return (parts[0] + parts[1]) + (parts[2] + parts[3]) if len(parts) == 4 else parts[0] + parts[1]

        members = rounds[turn][1]
        parts = [total] + [landed[turn, e] for e in range(len(group))]
        total = four(parts[:members])
        if len(parts) > members:
            total = total + four(parts[members:])
    quotient = total[:, 1:2] / total[:, 0:1]
    extra = jnp.zeros((deep - columns, BS), jnp.float32)

    def fill(n, carry):
        span = pl.ds(pl.multiple_of(n * BS, BS), BS)
        r = (image[:columns, span] - x_ref[:, span] * quotient) / jacobi[:, span]
        r_ref[:, span] = r
        window[n + 2] = jnp.concatenate([r, extra], axis=0).astype(jnp.bfloat16)
        return carry

    lax.fori_loop(0, nbr, fill, 0, unroll=2)
    halos = halo_copies(window, nbr, (end_send, end_recv), field, dom)
    start_halos(halos, dom, ends)
    copy = send_wet(
        lambda span: r_ref[:, span], columns, wide, rows, counts[0], coupling, rows_in, picked, outgoing, wet,
        (side_send, side_recv), (1 - field, dom),
    )
    finish_halos(halos, dom, ends)
    copy.wait()


def exchange_second(vec_modes, image, jacobi, wet_rows, wet_counts, coupling):
    columns, wide = vec_modes.shape
    slots = wet_rows.shape[1]
    bits = (lax.axis_size("dom") - 1).bit_length()
    rounds = [(1 << bit, 4 if bit + 1 < bits else 2) for bit in range(0, bits, 2)]
    most = 2 * rounds[0][1] - 1
    return pl.pallas_call(
        functools.partial(second_kernel, rounds),
        out_shape=(
            jax.ShapeDtypeStruct((wide // BS + 5, rows_deep(columns), BS), jnp.bfloat16),
            jax.ShapeDtypeStruct((slots, LANES), jnp.bfloat16),
            jax.ShapeDtypeStruct((columns, wide), jnp.float32),
        ),
        in_specs=[SMEM, SMEM, VMEM, VMEM, VMEM, VMEM],
        out_specs=(VMEM, VMEM, VMEM),
        scratch_shapes=exchange_scratch(wide, slots)
        + [
            pltpu.VMEM((len(rounds), columns, LANES), jnp.float32),
            pltpu.VMEM((len(rounds), most, columns, LANES), jnp.float32),
            pltpu.SemaphoreType.DMA((len(rounds), most)),
            pltpu.SemaphoreType.DMA((len(rounds), most)),
        ],
        compiler_params=pltpu.CompilerParams(
            collective_id=3, has_side_effects=True, vmem_limit_bytes=32 * 1024 * 1024
        ),
    )(wet_rows, wet_counts, coupling, vec_modes, image, jacobi)


def group_rows(kind_of, lists, nbr, types, cells):
    spare = nbr + 2
    for offset in range(3):
        for slot in range((cells + 1) * GROUP):
            lists[offset, slot] = spare
        known = [kind_of(offset, row) for row in range(2 - offset, nbr + 2)]
        place = jnp.int32(0)
        for kind in range(types):
            for row, found in enumerate(known):
                lists[offset, place] = row + 2 - offset
                place = place + (found == kind).astype(jnp.int32)
            for slot in range(GROUP):
                lists[offset, place + slot] = spare
            place = ((place + (GROUP - 1)) // GROUP) * GROUP


def operator_kernel(cells, with_diagonal, kinds, scales, rows, window, wet, tables, o_ref, *rest):
    if with_diagonal:
        jacobi, diagonal, total, rows_in, rows_out, lists = rest
    else:
        total, rows_in, rows_out, lists = rest
    columns, wide = o_ref.shape
    nbr = wide // BS
    types = tables.shape[1]
    deep = window.shape[1]
    slots = wet.shape[0]
    base = lax.axis_index("dom") * nbr - 2

    def kind_of(offset, row):
        return kinds[offset, jnp.maximum(base + row, 0)]

    def scale_of(offset, row):
        return scales[offset, jnp.maximum(base + row, 0)]

    group_rows(kind_of, lists, nbr, types, cells)

    def clear(n, carry):
        total[n] = jnp.zeros(total.shape[1:], jnp.float32)
        span = pl.ds(pl.multiple_of(n * BS, BS), BS)
        rows_out[span, :] = jnp.zeros((BS, LANES), jnp.float32)
        return carry

    lax.fori_loop(0, nbr, clear, 0)

    def widen(i, carry):
        span = pl.ds(pl.multiple_of(i * LANES, LANES), LANES)
        rows_in[span, :] = wet[span, :].astype(jnp.float32)
        return carry

    lax.fori_loop(0, slots // LANES, widen, 0, unroll=4)

    def scatter(i, carry):
        for slot in range(UNROLL):
            at = i * UNROLL + slot
            rows_out[pl.ds(rows[0, at], 1), :] = rows_in[pl.ds(at, 1), :]
        return carry

    lax.fori_loop(0, slots // UNROLL, scatter, 0)
    if with_diagonal:
        eye = lax.broadcasted_iota(jnp.int32, (LANES, LANES), 0) == lax.broadcasted_iota(
            jnp.int32, (LANES, LANES), 1
        )
        for kind in range(types):
            for part in range(BS // LANES):
                span = slice(part * LANES, (part + 1) * LANES)
                cell = tables[0, kind, span, span].astype(jnp.float32)
                diagonal[kind, :, span] = jnp.sum(jnp.where(eye, cell, 0.0), axis=0, keepdims=True)
        for n in range(nbr):
            jacobi[:, n * BS : (n + 1) * BS] = scale_of(0, n + 2) * diagonal[kind_of(0, n + 2)]

    def step(i, carry):
        for offset in range(3):
            found = [lists[offset, i * GROUP + u] for u in range(GROUP)]
            held = [jnp.minimum(row, nbr + 1) for row in found]
            kind = kind_of(offset, held[0])
            factors = [scale_of(offset, row) for row in held]
            for ahead in (True, False) if offset else (True,):
                if ahead:
                    sources = [row + offset for row in found]
                    targets = [jnp.where(row < 2, nbr, row - 2) for row in found]
                else:
                    sources = found
                    targets = [jnp.minimum(row - 2 + offset, nbr) for row in found]
                left = jnp.concatenate([window[source] for source in sources], axis=0)
                product = lax.dot_general(
                    left,
                    tables[offset, kind],
                    NT if ahead and offset else NN,
                    preferred_element_type=jnp.float32,
                )
                for u in range(GROUP):
                    total[targets[u]] += factors[u] * product[u * deep : (u + 1) * deep]
        return carry

    lax.fori_loop(0, cells, step, 0)
    parts = BS // LANES

    def turn_out(n, carry):
        for part in range(parts):
            span = pl.ds(pl.multiple_of(n * BS + part * LANES, LANES), LANES)
            inner = slice(part * LANES, (part + 1) * LANES)
            o_ref[:, span] = total[n, :columns, inner] + rows_out[span, :].T[:columns]
        return carry

    lax.fori_loop(0, nbr, turn_out, 0, unroll=4)


def operate(columns, window, wet, kinds, scales, rows, tables, with_diagonal):
    nbr = window.shape[0] - 5
    wide = nbr * BS
    deep = window.shape[1]
    slots = wet.shape[0]
    types = tables.shape[1]
    cells = (nbr + 2 + types * (GROUP - 1)) // GROUP
    outs = [jax.ShapeDtypeStruct((columns, wide), jnp.float32)]
    scratch = [
        pltpu.VMEM((nbr + 1, deep, BS), jnp.float32),
        pltpu.VMEM((slots, LANES), jnp.float32),
        pltpu.VMEM((wide, LANES), jnp.float32),
        pltpu.SMEM((3, (cells + 1) * GROUP), jnp.int32),
    ]
    if with_diagonal:
        outs.append(jax.ShapeDtypeStruct((1, wide), jnp.float32))
        scratch = [pltpu.VMEM((types, 1, BS), jnp.float32)] + scratch
    return pl.pallas_call(
        functools.partial(operator_kernel, cells, with_diagonal),
        out_shape=tuple(outs),
        in_specs=[SMEM, SMEM, SMEM, VMEM, VMEM, VMEM],
        out_specs=(VMEM,) * len(outs),
        scratch_shapes=scratch,
        cost_estimate=pl.CostEstimate(
            flops=10 * columns * wide * BS, bytes_accessed=16 * columns * wide, transcendentals=0
        ),
        compiler_params=pltpu.CompilerParams(vmem_limit_bytes=32 * 1024 * 1024),
    )(kinds, scales, rows, window, wet, tables)


def shards(modes, previous, kinds, scales, tables, wet_rows, wet_counts, coupling):
    high = lax.Precision.HIGH
    vec_modes = modes[0]
    vec_prev = previous[0]
    columns, wide = vec_modes.shape
    shared = (kinds[0], scales[0], wet_rows, tables[0])
    weights = coupling.reshape(-1, LANES)
    window, wet = exchange_first(vec_modes, vec_prev, wet_rows, wet_counts, weights)
    image_pair, jacobi = operate(2 * columns, window, wet, *shared, True)
    image_x, image_p = image_pair[:columns], image_pair[columns:]
    window, wet, residual_dir = exchange_second(vec_modes, image_pair, jacobi, wet_rows, wet_counts, weights)
    (image_r,) = operate(columns, window, wet, *shared, False)
    search = jnp.concatenate([vec_modes, residual_dir, vec_prev], axis=0)
    image_all = jnp.concatenate([image_x, image_r, image_p], axis=0)
    ndof = 2.0 * lax.axis_size("dom") * wide
    part_b = jnp.dot(search, search.T, precision=high)
    part_a = jnp.dot(search, image_all.T, precision=high)
    part_a = part_a + part_a.T
    size = 3 * columns
    row = lax.broadcasted_iota(jnp.int32, (size, size + 8), 0)
    col = lax.broadcasted_iota(jnp.int32, (size, size + 8), 1)
    packed = jnp.where(
        col <= row,
        jnp.pad(part_b, ((0, 0), (0, 8))),
        jnp.pad(part_a, ((0, 0), (1, 7))),
    )
    half = -(-size // 16) * 8
    packed = jnp.pad(packed, ((0, 2 * half - size), (0, 0))).reshape(2, half, size + 8)
    packed = summed_everywhere(packed, 2).reshape(2 * half, size + 8)
    return finish(packed, vec_modes, residual_dir, vec_prev, ndof)


def solution(mesh):
    return jax.shard_map(
        shards,
        mesh=mesh,
        in_specs=(
            P("field", None, "dom"),
            P("field", None, "dom"),
            P("field", None, None),
            P("field", None, None),
            P("field", None, None, None, None),
            P("field", "dom"),
            P("dom"),
            P("dom"),
        ),
        out_specs=(P("field", None, "dom"), P()),
        check_vma=False,
    )
```

```python
import functools

import jax
import jax.numpy as jnp
from jax import lax
from jax.experimental import pallas as pl
from jax.experimental.pallas import tpu as pltpu
from jax.sharding import PartitionSpec as P

BS = 512
LANES = 128
GROUP = 4
UNROLL = 64
PARTS = 4
SPAN = 2048
MESH = pl.DeviceIdType.MESH
NN = (((1,), (0,)), ((), ()))
NT = (((1,), (1,)), ((), ()))


SUB = 8


def split_dot(left, right, dims):
    lh = left.astype(jnp.bfloat16)
    ll = (left - lh.astype(jnp.float32)).astype(jnp.bfloat16)
    rh = right.astype(jnp.bfloat16)
    rl = (right - rh.astype(jnp.float32)).astype(jnp.bfloat16)

    def dot(a, b):
        return lax.dot_general(a, b, dims, preferred_element_type=jnp.float32)

    return dot(lh, rh) + (dot(lh, rl) + dot(ll, rh))


def eliminate(gram, size, inverse_ref):
    panels = size // SUB
    sub = lax.broadcasted_iota(jnp.int32, (SUB, LANES), 0)
    lane = lax.broadcasted_iota(jnp.int32, (SUB, LANES), 1)
    left = [gram[SUB * i : SUB * (i + 1)] for i in range(panels)]
    right = [(lane == sub + SUB * i).astype(jnp.float32) for i in range(panels)]

    def over_lanes(cell, column):
        return jnp.broadcast_to(cell[:, column : column + 1], (SUB, LANES))

    def over_rows(cell, row):
        return jnp.broadcast_to(cell[row : row + 1], (SUB, LANES))

    for k in range(panels):
        columns = [over_lanes(left[k], SUB * k + c) for c in range(SUB)]
        cells = [left[k], right[k]]
        for c in range(SUB):
            pivot = over_rows(columns[c], c)
            inverse = 1.0 / pivot
            inverse_ref[SUB * k + c : SUB * k + c + 1] = (cells[1] * lax.rsqrt(pivot))[c : c + 1]
            here = sub == c
            factor = columns[c]

            def reduced(cell):
                row = over_rows(cell, c) * inverse
                return jnp.where(here, row, cell - factor * row)

            for later in range(c + 1, SUB):
                columns[later] = reduced(columns[later])
            cells = [reduced(cell) for cell in cells]
        rows = [[over_rows(cell, c) for c in range(SUB)] for cell in cells]
        for i in range(k + 1, panels):
            source = left[i]
            for c in range(SUB):
                factor = over_lanes(source, SUB * k + c)
                left[i] = left[i] - factor * rows[0][c]
                right[i] = right[i] - factor * rows[1][c]


def finish_kernel(chunk, scale, packed_ref, x_ref, r_ref, p_ref, basis_ref, projected_ref, inverse_ref, held, sems):
    columns, wide = x_ref.shape
    size = 3 * columns
    packed = packed_ref[...] * scale
    row = lax.broadcasted_iota(jnp.int32, packed.shape, 0)
    col = lax.broadcasted_iota(jnp.int32, packed.shape, 1)
    gram_b = jnp.where(col <= row, packed, packed.T)
    inverse_ref[...] = jnp.zeros_like(inverse_ref)
    eliminate(gram_b, size, inverse_ref)
    high = jnp.concatenate([packed[:, 1:], packed[:, :1]], axis=1)
    gram_a = jnp.where(col >= row, high, high.T)
    gram_a = jnp.where(jnp.maximum(row, col) < size, 0.5 * gram_a, 0.0)
    inverse = inverse_ref[...]
    projected = split_dot(split_dot(inverse, gram_a, NN), inverse, NT)
    projected_ref[...] = projected[:size, :size]
    ih = inverse.astype(jnp.bfloat16)
    il = (inverse - ih.astype(jnp.float32)).astype(jnp.bfloat16)
    twice = jnp.concatenate([ih, ih], axis=1)
    blank = jnp.zeros((LANES - size, chunk), jnp.float32)

    def copy(n):
        span = pl.ds(pl.multiple_of(n * chunk, chunk), chunk)
        return pltpu.make_async_copy(held.at[n], basis_ref.at[0, :, span], sems.at[n])

    def step(n, carry):
        span = pl.ds(pl.multiple_of(n * chunk, chunk), chunk)
        search = jnp.concatenate([x_ref[:, span], r_ref[:, span], p_ref[:, span], blank], axis=0)
        sh = search.astype(jnp.bfloat16)
        sl = (search - sh.astype(jnp.float32)).astype(jnp.bfloat16)
        both = jnp.concatenate([sh, sl], axis=0)
        out = lax.dot_general(twice, both, NN, preferred_element_type=jnp.float32)
        out = out + lax.dot_general(il, sh, NN, preferred_element_type=jnp.float32)
        held[n] = out[:size]
        copy(n).start()
        return carry

    lax.fori_loop(0, wide // chunk, step, 0)

    def close(n, carry):
        copy(n).wait()
        return carry

    lax.fori_loop(0, wide // chunk, close, 0)


def finish(packed, vec_modes, residual_dir, vec_prev, ndof):
    columns, wide = vec_modes.shape
    size = 3 * columns
    chunk = min(512, wide)
    vmem = pl.BlockSpec(memory_space=pltpu.VMEM)
    return pl.pallas_call(
        functools.partial(finish_kernel, chunk, 1.0 / ndof),
        out_shape=(
            jax.ShapeDtypeStruct((1, size, wide), jnp.float32),
            jax.ShapeDtypeStruct((size, size), jnp.float32),
        ),
        in_specs=[vmem, vmem, vmem, vmem],
        out_specs=(pl.BlockSpec(memory_space=pl.ANY), vmem),
        scratch_shapes=[
            pltpu.VMEM((LANES, LANES), jnp.float32),
            pltpu.VMEM((wide // chunk, size, chunk), jnp.float32),
            pltpu.SemaphoreType.DMA((wide // chunk,)),
        ],
        cost_estimate=pl.CostEstimate(
            flops=6 * size * size * wide, bytes_accessed=8 * size * wide, transcendentals=0
        ),
        compiler_params=pltpu.CompilerParams(vmem_limit_bytes=24 * 1024 * 1024),
    )(packed, vec_modes, residual_dir, vec_prev)


def remote(source, target, sems, peer):
    return pltpu.make_async_remote_copy(
        src_ref=source,
        dst_ref=target,
        send_sem=sems[0],
        recv_sem=sems[1],
        device_id=peer,
        device_id_type=MESH,
    )


def greet(peers):
    barrier = pltpu.get_barrier_semaphore()
    for peer in peers:
        pl.semaphore_signal(barrier, inc=1, device_id=peer, device_id_type=MESH)


def greet_ends(field, dom, ends):
    barrier = pltpu.get_barrier_semaphore()

    @pl.when(dom > 0)
    def _():
        pl.semaphore_signal(barrier, inc=1, device_id=(field, dom - 1), device_id_type=MESH)

    @pl.when(dom < ends)
    def _():
        pl.semaphore_signal(barrier, inc=1, device_id=(field, dom + 1), device_id_type=MESH)


def meet(dom, ends, count):
    left = (dom + ends - 1) // ends
    right = (2 * ends - dom - 1) // ends
    pl.semaphore_wait(pltpu.get_barrier_semaphore(), count + left + right)


def clear_ends(window, nbr):
    empty = jnp.zeros((2,) + window.shape[1:], window.dtype)
    window[:2] = empty
    window[nbr + 2 : nbr + 4] = empty


def halo_copies(window, nbr, sems, field, dom):
    send, recv = sems
    left = remote(
        window.at[pl.ds(2, 2)], window.at[pl.ds(nbr + 2, 2)], (send.at[0], recv.at[0]), (field, dom - 1)
    )
    right = remote(
        window.at[pl.ds(nbr, 2)], window.at[pl.ds(0, 2)], (send.at[1], recv.at[1]), (field, dom + 1)
    )
    return left, right


def start_halos(copies, dom, ends):
    left, right = copies

    @pl.when(dom > 0)
    def _():
        left.start()

    @pl.when(dom < ends)
    def _():
        right.start()


def finish_halos(copies, dom, ends):
    left, right = copies

    @pl.when(dom > 0)
    def _():
        left.wait_send()
        right.wait_recv()

    @pl.when(dom < ends)
    def _():
        right.wait_send()
        left.wait_recv()


def send_wet(read, columns, wide, rows, count, coupling, rows_in, picked, outgoing, wet, sems, peer):
    slots = picked.shape[0]
    blank = jnp.zeros((LANES - columns, LANES), jnp.float32)

    def turn_in(tile, carry):
        span = pl.ds(pl.multiple_of(tile * LANES, LANES), LANES)
        rows_in[span, :] = jnp.concatenate([read(span), blank], axis=0).T
        return carry

    lax.fori_loop(0, wide // LANES, turn_in, 0, unroll=16)

    def gather(i, carry):
        for slot in range(UNROLL):
            at = i * UNROLL + slot
            picked[pl.ds(at, 1), :] = rows_in[pl.ds(rows[0, at], 1), :]
        return carry

    lax.fori_loop(0, slots // UNROLL, gather, 0)

    def weigh(i, carry):
        span = pl.ds(pl.multiple_of(i * LANES, LANES), LANES)
        used = i * LANES + lax.broadcasted_iota(jnp.int32, (1, LANES), 1) < count
        weights = jnp.where(used, coupling[pl.ds(i, 1), :], 0.0)
        spread = jnp.broadcast_to(weights, (LANES, LANES)).T
        outgoing[span, :] = (picked[span, :] * spread).astype(jnp.bfloat16)
        return carry

    cells = slots // LANES
    copies = []
    for part in range(PARTS):
        low, high = cells * part // PARTS, cells * (part + 1) // PARTS
        lax.fori_loop(low, high, weigh, 0, unroll=2)
        span = pl.ds(low * LANES, (high - low) * LANES)
        copy = remote(outgoing.at[span], wet.at[span], (sems[0].at[part], sems[1].at[part]), peer)
        copy.start()
        copies.append(copy)
    return copies


def first_kernel(
    counts, rows_in_hbm, coupling_in, x_in, p_in, tables_in, window, wet, x_ref, p_ref, tables, coupling,
    rows_in, picked, outgoing, side_send, side_recv, end_send, end_recv, rows, loads,
):
    field = lax.axis_index("field")
    dom = lax.axis_index("dom")
    ends = lax.axis_size("dom") - 1
    columns, wide = x_ref.shape
    nbr = wide // BS
    pairs = [(x_in.at[0], x_ref), (p_in.at[0], p_ref), (rows_in_hbm, rows), (coupling_in, coupling), (tables_in.at[0], tables)]
    arrivals = [pltpu.make_async_copy(source, target, loads.at[n]) for n, (source, target) in enumerate(pairs)]
    for arrival in arrivals:
        arrival.start()
    clear_ends(window, nbr)
    greet([(1 - field, dom)])
    greet_ends(field, dom, ends)

    def read(span):
        return jnp.concatenate([x_ref[:, span], p_ref[:, span]], axis=0)

    def fill(n, carry):
        span = pl.ds(pl.multiple_of(n * BS, BS), BS)
        window[n + 2] = read(span).astype(jnp.bfloat16)
        return carry

    arrivals[0].wait()
    arrivals[1].wait()
    lax.fori_loop(0, nbr, fill, 0, unroll=2)
    meet(dom, ends, 1)
    halos = halo_copies(window, nbr, (end_send, end_recv), field, dom)
    start_halos(halos, dom, ends)
    arrivals[2].wait()
    arrivals[3].wait()
    copies = send_wet(
        read, 2 * columns, wide, rows, counts[0], coupling, rows_in, picked, outgoing, wet,
        (side_send, side_recv), (1 - field, dom),
    )
    arrivals[4].wait()
    finish_halos(halos, dom, ends)
    for copy in copies:
        copy.wait()


def exchange_scratch(wide, slots):
    return [
        pltpu.VMEM((wide, LANES), jnp.float32),
        pltpu.VMEM((slots, LANES), jnp.float32),
        pltpu.VMEM((slots, LANES), jnp.bfloat16),
        pltpu.SemaphoreType.DMA((PARTS,)),
        pltpu.SemaphoreType.DMA((PARTS,)),
        pltpu.SemaphoreType.DMA((2,)),
        pltpu.SemaphoreType.DMA((2,)),
    ]


def rows_deep(columns):
    return -(-columns // 16) * 16


SMEM = pl.BlockSpec(memory_space=pltpu.SMEM)
VMEM = pl.BlockSpec(memory_space=pltpu.VMEM)
HBM = pl.BlockSpec(memory_space=pltpu.HBM)


def exchange_first(modes, previous, wet_rows, wet_counts, coupling, tables):
    _, columns, wide = modes.shape
    slots = wet_rows.shape[1]
    held = jax.ShapeDtypeStruct((columns, wide), jnp.float32)
    return pl.pallas_call(
        first_kernel,
        out_shape=(
            jax.ShapeDtypeStruct((wide // BS + 5, rows_deep(2 * columns), BS), jnp.bfloat16),
            jax.ShapeDtypeStruct((slots, LANES), jnp.bfloat16),
            held,
            held,
            jax.ShapeDtypeStruct(tables.shape[1:], tables.dtype),
            jax.ShapeDtypeStruct(coupling.shape, coupling.dtype),
        ),
        in_specs=[SMEM, HBM, HBM, HBM, HBM, HBM],
        out_specs=(VMEM,) * 6,
        scratch_shapes=exchange_scratch(wide, slots)
        + [pltpu.SMEM(wet_rows.shape, jnp.int32), pltpu.SemaphoreType.DMA((5,))],
        compiler_params=pltpu.CompilerParams(
            collective_id=1, has_side_effects=True, vmem_limit_bytes=24 * 1024 * 1024
        ),
    )(wet_counts, wet_rows, coupling, modes, previous, tables)


def gram_part(left, right):
    lh = left.astype(jnp.bfloat16)
    ll = (left - lh.astype(jnp.float32)).astype(jnp.bfloat16)
    rh = right.astype(jnp.bfloat16)
    rl = (right - rh.astype(jnp.float32)).astype(jnp.bfloat16)
    rows = left.shape[0]
    both = lax.dot_general(
        jnp.concatenate([lh, ll], axis=0), rh, NT, preferred_element_type=jnp.float32
    )
    cross = lax.dot_general(lh, rl, NT, preferred_element_type=jnp.float32)
    return both[:rows] + (both[rows:] + cross)


def gram_over(low, high, step, read_left, read_right, out):
    def add(n, carry):
        span = pl.ds(pl.multiple_of(n * step, step), step)
        out[...] += gram_part(read_left(span), read_right(span))
        return carry

    lax.fori_loop(low, high, add, 0)


def neighbours(rounds, field, dom):
    groups = []
    for turn, (step, members) in enumerate(rounds):
        low = (1 - 2 * ((dom // step) % 2)) * step
        high = (1 - 2 * ((dom // (2 * step)) % 2)) * 2 * step
        group = [(field, dom + (e % 2) * low + (e // 2) * high) for e in range(members)]
        across = [(1 - field, there) for _, there in group] if turn == 0 else []
        groups.append(group[1:] + across)
    return groups


def gathered(total, landed, members):
    def fold(parts):
        if len(parts) == 4:
            return (parts[0] + parts[1]) + (parts[2] + parts[3])
        return parts[0] + parts[1]

    parts = [total] + landed
    total = fold(parts[:members])
    return total + fold(parts[members:]) if len(parts) > members else total


def sum_rounds():
    bits = (lax.axis_size("dom") - 1).bit_length()
    return [(1 << bit, 4 if bit + 1 < bits else 2) for bit in range(0, bits, 2)]


def second_kernel(
    rounds, rows, counts, coupling, x_ref, p_ref, image, jacobi, window, wet, r_ref, gram,
    rows_in, picked, outgoing, side_send, side_recv, end_send, end_recv, held, landed, sum_send, sum_recv,
):
    field = lax.axis_index("field")
    dom = lax.axis_index("dom")
    ends = lax.axis_size("dom") - 1
    columns, wide = x_ref.shape
    nbr = wide // BS
    deep = window.shape[1]
    groups = neighbours(rounds, field, dom)
    clear_ends(window, nbr)
    peers = [peer for group in groups for peer in group]
    greet(peers)
    greet_ends(field, dom, ends)

    def add(n, carry):
        span = pl.ds(pl.multiple_of(n * LANES, LANES), LANES)
        x = x_ref[:, span]
        return carry[0] + x * x, carry[1] + x * image[:columns, span]

    zero = jnp.zeros((columns, LANES), jnp.float32)
    squares, products = lax.fori_loop(0, wide // LANES, add, (zero, zero), unroll=8)
    lane = lax.broadcasted_iota(jnp.int32, (columns, LANES), 1)
    total = jnp.where(
        lane == 0,
        jnp.sum(squares, axis=1, keepdims=True),
        jnp.where(lane == 1, jnp.sum(products, axis=1, keepdims=True), 0.0),
    )
    total = jnp.concatenate([total, jnp.zeros((LANES - columns, LANES), jnp.float32)], axis=0).T[:SUB]
    gram[...] = jnp.zeros_like(gram)
    meet(dom, ends, len(peers))
    pieces = wide // SPAN
    for turn, group in enumerate(groups):
        held[turn] = total
        copies = [
            remote(held.at[turn], landed.at[turn, e], (sum_send.at[turn, e], sum_recv.at[turn, e]), peer)
            for e, peer in enumerate(group)
        ]
        for copy in copies:
            copy.start()
        gram_over(
            pieces * turn // len(groups),
            pieces * (turn + 1) // len(groups),
            SPAN,
            lambda span: jnp.concatenate([x_ref[:, span], p_ref[:, span]], axis=0),
            lambda span: jnp.concatenate([x_ref[:, span], p_ref[:, span], image[:, span]], axis=0),
            gram,
        )
        for copy in copies:
            copy.wait()
        members = rounds[turn][1]
        total = gathered(total, [landed[turn, e] for e in range(len(group))], members)
    total = jnp.concatenate([total, jnp.zeros((LANES - SUB, LANES), jnp.float32)], axis=0).T[:columns]
    quotient = total[:, 1:2] / total[:, 0:1]
    extra = jnp.zeros((deep - columns, BS), jnp.float32)

    def fill(n, carry):
        span = pl.ds(pl.multiple_of(n * BS, BS), BS)
        r = (image[:columns, span] - x_ref[:, span] * quotient) / jacobi[:, span]
        r_ref[:, span] = r
        window[n + 2] = jnp.concatenate([r, extra], axis=0).astype(jnp.bfloat16)
        return carry

    lax.fori_loop(0, nbr, fill, 0, unroll=2)
    halos = halo_copies(window, nbr, (end_send, end_recv), field, dom)
    start_halos(halos, dom, ends)
    copies = send_wet(
        lambda span: r_ref[:, span], columns, wide, rows, counts[0], coupling, rows_in, picked, outgoing, wet,
        (side_send, side_recv), (1 - field, dom),
    )
    finish_halos(halos, dom, ends)
    for copy in copies:
        copy.wait()


def exchange_second(vec_modes, vec_prev, image, jacobi, wet_rows, wet_counts, coupling):
    columns, wide = vec_modes.shape
    slots = wet_rows.shape[1]
    rounds = sum_rounds()
    most = 2 * rounds[0][1] - 1
    return pl.pallas_call(
        functools.partial(second_kernel, rounds),
        out_shape=(
            jax.ShapeDtypeStruct((wide // BS + 5, rows_deep(columns), BS), jnp.bfloat16),
            jax.ShapeDtypeStruct((slots, LANES), jnp.bfloat16),
            jax.ShapeDtypeStruct((columns, wide), jnp.float32),
            jax.ShapeDtypeStruct((2 * columns, 4 * columns), jnp.float32),
        ),
        in_specs=[SMEM, SMEM, VMEM, VMEM, VMEM, VMEM, VMEM],
        out_specs=(VMEM,) * 4,
        scratch_shapes=exchange_scratch(wide, slots)
        + [
            pltpu.VMEM((len(rounds), SUB, LANES), jnp.float32),
            pltpu.VMEM((len(rounds), most, SUB, LANES), jnp.float32),
            pltpu.SemaphoreType.DMA((len(rounds), most)),
            pltpu.SemaphoreType.DMA((len(rounds), most)),
        ],
        compiler_params=pltpu.CompilerParams(
            collective_id=3, has_side_effects=True, vmem_limit_bytes=20 * 1024 * 1024
        ),
    )(wet_rows, wet_counts, coupling, vec_modes, vec_prev, image, jacobi)


def gram_kernel(
    rounds, x_ref, p_ref, r_ref, image, image_r, known, o_ref,
    fresh, gram_b, gram_a, packed, held, landed, across, send_sem, recv_sem, side_send, side_recv,
):
    field = lax.axis_index("field")
    dom = lax.axis_index("dom")
    columns, wide = x_ref.shape
    groups = []
    for step, members in rounds:
        low = (1 - 2 * ((dom // step) % 2)) * step
        high = (1 - 2 * ((dom // (2 * step)) % 2)) * 2 * step
        groups.append([dom + (e % 2) * low + (e // 2) * high for e in range(1, members)])
    peers = [(1 - field, dom)] + [(field, peer) for group in groups for peer in group]
    greet(peers)
    fresh[...] = jnp.zeros_like(fresh)
    gram_over(
        0,
        wide // SPAN,
        SPAN,
        lambda span: jnp.concatenate([r_ref[:, span], image_r[:, span]], axis=0),
        lambda span: jnp.concatenate(
            [x_ref[:, span], p_ref[:, span], r_ref[:, span], image[:, span], image_r[:, span]], axis=0
        ),
        fresh,
    )
    n = columns
    new = fresh[...]
    old = known[...]
    turned = jnp.concatenate(
        [new[:, : 2 * n], jnp.zeros((2 * n, LANES - 2 * n), jnp.float32)], axis=1
    )
    turned = jnp.concatenate([turned, jnp.zeros((LANES - 2 * n, LANES), jnp.float32)], axis=0).T
    gram_b[...] = jnp.zeros_like(gram_b)
    gram_a[...] = jnp.zeros_like(gram_a)
    x, r, p = slice(0, n), slice(n, 2 * n), slice(2 * n, 3 * n)
    gram_b[x, x] = old[:n, :n]
    gram_b[r, x] = new[:n, :n]
    gram_b[r, r] = new[:n, 2 * n : 3 * n]
    gram_b[p, x] = old[n:, :n]
    gram_b[p, r] = turned[n : 2 * n, :n]
    gram_b[p, p] = old[n:, n : 2 * n]
    gram_a[x, x] = old[:n, 2 * n : 3 * n]
    gram_a[x, r] = turned[:n, n : 2 * n]
    gram_a[x, p] = old[:n, 3 * n :]
    gram_a[r, x] = new[:n, 3 * n : 4 * n]
    gram_a[r, r] = new[:n, 5 * n :]
    gram_a[r, p] = new[:n, 4 * n : 5 * n]
    gram_a[p, x] = old[n:, 2 * n : 3 * n]
    gram_a[p, r] = turned[n : 2 * n, n : 2 * n]
    gram_a[p, p] = old[n:, 3 * n :]
    both = gram_a[...] + gram_a[...].T
    both = jnp.concatenate([both[:, LANES - 1 :], both[:, : LANES - 1]], axis=1)
    row = lax.broadcasted_iota(jnp.int32, (LANES, LANES), 0)
    col = lax.broadcasted_iota(jnp.int32, (LANES, LANES), 1)
    half = LANES // 2
    whole = jnp.where(col <= row, gram_b[...], both)
    packed[0] = whole[:half]
    packed[1] = whole[half:]
    pl.semaphore_wait(pltpu.get_barrier_semaphore(), len(peers))
    copy = remote(packed.at[1 - field], across.at[0], (side_send.at[0], side_recv.at[0]), (1 - field, dom))
    copy.start()
    copy.wait()
    total = packed[field] + across[0]
    for turn, group in enumerate(groups):
        held[turn] = total
        copies = [
            remote(
                held.at[turn], landed.at[turn, e], (send_sem.at[turn, e], recv_sem.at[turn, e]), (field, peer)
            )
            for e, peer in enumerate(group)
        ]
        for copy in copies:
            copy.start()
        for copy in copies:
            copy.wait()
        total = gathered(total, [landed[turn, e] for e in range(len(group))], rounds[turn][1])
    o_ref[field] = total
    held[len(groups)] = total
    copy = remote(held.at[len(groups)], across.at[1], (side_send.at[1], side_recv.at[1]), (1 - field, dom))
    copy.start()
    copy.wait()
    o_ref[1 - field] = across[1]


def gram_everywhere(vec_modes, vec_prev, residual_dir, image, image_r, known):
    columns = vec_modes.shape[0]
    rounds = sum_rounds()
    slots = len(rounds)
    cell = (LANES // 2, LANES)
    return pl.pallas_call(
        functools.partial(gram_kernel, rounds),
        out_shape=jax.ShapeDtypeStruct((2,) + cell, jnp.float32),
        in_specs=[VMEM] * 6,
        out_specs=VMEM,
        scratch_shapes=[
            pltpu.VMEM((2 * columns, 6 * columns), jnp.float32),
            pltpu.VMEM((LANES, LANES), jnp.float32),
            pltpu.VMEM((LANES, LANES), jnp.float32),
            pltpu.VMEM((2,) + cell, jnp.float32),
            pltpu.VMEM((slots + 1,) + cell, jnp.float32),
            pltpu.VMEM((slots, 3) + cell, jnp.float32),
            pltpu.VMEM((2,) + cell, jnp.float32),
            pltpu.SemaphoreType.DMA((slots, 3)),
            pltpu.SemaphoreType.DMA((slots, 3)),
            pltpu.SemaphoreType.DMA((2,)),
            pltpu.SemaphoreType.DMA((2,)),
        ],
        compiler_params=pltpu.CompilerParams(
            collective_id=2, has_side_effects=True, vmem_limit_bytes=16 * 1024 * 1024
        ),
    )(vec_modes, vec_prev, residual_dir, image, image_r, known)


def group_rows(kind_of, lists, nbr, types, cells):
    spare = nbr + 2
    bits = 32 // types
    mask = (1 << bits) - 1
    for offset in range(3):
        for slot in range(cells * GROUP):
            lists[offset, slot] = spare
        first = 2 - offset
        shifts = [kind_of(offset, row) * bits for row in range(first, nbr + 2)]
        count = jnp.int32(0)
        ranks = []
        for shift in shifts:
            ranks.append(lax.shift_right_logical(count, shift) & mask)
            count = count + lax.shift_left(jnp.int32(1), shift)
        starts = jnp.int32(0)
        place = jnp.int32(0)
        for kind in range(types):
            starts = starts + place * (1 << bits * kind)
            here = lax.shift_right_logical(count, jnp.int32(bits * kind)) & mask
            place = place + ((here + (GROUP - 1)) & -GROUP)
        for n, (shift, rank) in enumerate(zip(shifts, ranks)):
            lists[offset, (lax.shift_right_logical(starts, shift) & mask) + rank] = n + first


def operator_kernel(cells, with_diagonal, kinds, scales, rows, window, wet, tables, o_ref, *rest):
    if with_diagonal:
        jacobi, diagonal, total, rows_in, rows_out, lists = rest
    else:
        total, rows_in, rows_out, lists = rest
    columns, wide = o_ref.shape
    nbr = wide // BS
    types = tables.shape[1]
    deep = window.shape[1]
    slots = wet.shape[0]
    base = lax.axis_index("dom") * nbr - 2

    def kind_of(offset, row):
        return kinds[offset, jnp.maximum(base + row, 0)]

    def scale_of(offset, row):
        return scales[offset, jnp.maximum(base + row, 0)]

    group_rows(kind_of, lists, nbr, types, cells)

    def clear(n, carry):
        total[n] = jnp.zeros(total.shape[1:], jnp.float32)
        span = pl.ds(pl.multiple_of(n * BS, BS), BS)
        rows_out[span, :] = jnp.zeros((BS, LANES), jnp.float32)
        return carry

    lax.fori_loop(0, nbr, clear, 0)

    def widen(i, carry):
        span = pl.ds(pl.multiple_of(i * LANES, LANES), LANES)
        rows_in[span, :] = wet[span, :].astype(jnp.float32)
        return carry

    lax.fori_loop(0, slots // LANES, widen, 0, unroll=4)

    def scatter(i, carry):
        for slot in range(UNROLL):
            at = i * UNROLL + slot
            rows_out[pl.ds(rows[0, at], 1), :] = rows_in[pl.ds(at, 1), :]
        return carry

    lax.fori_loop(0, slots // UNROLL, scatter, 0)
    if with_diagonal:
        eye = lax.broadcasted_iota(jnp.int32, (LANES, LANES), 0) == lax.broadcasted_iota(
            jnp.int32, (LANES, LANES), 1
        )
        for kind in range(types):
            for part in range(BS // LANES):
                span = slice(part * LANES, (part + 1) * LANES)
                cell = tables[0, kind, span, span].astype(jnp.float32)
                diagonal[kind, :, span] = jnp.sum(jnp.where(eye, cell, 0.0), axis=0, keepdims=True)
        for n in range(nbr):
            jacobi[:, n * BS : (n + 1) * BS] = scale_of(0, n + 2) * diagonal[kind_of(0, n + 2)]

    def step(i, carry):
        for offset in range(3):
            found = [lists[offset, i * GROUP + u] for u in range(GROUP)]
            held = [jnp.minimum(row, nbr + 1) for row in found]
            kind = kind_of(offset, held[0])
            factors = [scale_of(offset, row) for row in held]
            for ahead in (True, False) if offset else (True,):
                if ahead:
                    sources = [row + offset for row in found]
                    targets = [jnp.where(row < 2, nbr, row - 2) for row in found]
                else:
                    sources = found
                    targets = [jnp.minimum(row - 2 + offset, nbr) for row in found]
                left = jnp.concatenate([window[source] for source in sources], axis=0)
                product = lax.dot_general(
                    left,
                    tables[offset, kind],
                    NT if ahead and offset else NN,
                    preferred_element_type=jnp.float32,
                )
                for u in range(GROUP):
                    total[targets[u]] += factors[u] * product[u * deep : (u + 1) * deep]
        return carry

    lax.fori_loop(0, cells, step, 0)
    parts = BS // LANES

    def turn_out(n, carry):
        for part in range(parts):
            span = pl.ds(pl.multiple_of(n * BS + part * LANES, LANES), LANES)
            inner = slice(part * LANES, (part + 1) * LANES)
            o_ref[:, span] = total[n, :columns, inner] + rows_out[span, :].T[:columns]
        return carry

    lax.fori_loop(0, nbr, turn_out, 0, unroll=4)


def operate(columns, window, wet, kinds, scales, rows, tables, with_diagonal):
    nbr = window.shape[0] - 5
    wide = nbr * BS
    deep = window.shape[1]
    slots = wet.shape[0]
    types = tables.shape[1]
    cells = (nbr + 2 + types * (GROUP - 1)) // GROUP
    outs = [jax.ShapeDtypeStruct((columns, wide), jnp.float32)]
    scratch = [
        pltpu.VMEM((nbr + 1, deep, BS), jnp.float32),
        pltpu.VMEM((slots, LANES), jnp.float32),
        pltpu.VMEM((wide, LANES), jnp.float32),
        pltpu.SMEM((3, cells * GROUP), jnp.int32),
    ]
    if with_diagonal:
        outs.append(jax.ShapeDtypeStruct((1, wide), jnp.float32))
        scratch = [pltpu.VMEM((types, 1, BS), jnp.float32)] + scratch
    return pl.pallas_call(
        functools.partial(operator_kernel, cells, with_diagonal),
        out_shape=tuple(outs),
        in_specs=[SMEM, SMEM, SMEM, VMEM, VMEM, VMEM],
        out_specs=(VMEM,) * len(outs),
        scratch_shapes=scratch,
        cost_estimate=pl.CostEstimate(
            flops=10 * columns * wide * BS, bytes_accessed=16 * columns * wide, transcendentals=0
        ),
        compiler_params=pltpu.CompilerParams(vmem_limit_bytes=24 * 1024 * 1024),
    )(kinds, scales, rows, window, wet, tables)


def shards(modes, previous, kinds, scales, tables, wet_rows, wet_counts, coupling):
    _, columns, wide = modes.shape
    window, wet, vec_modes, vec_prev, field_tables, weights = exchange_first(
        modes, previous, wet_rows, wet_counts, coupling.reshape(-1, LANES), tables
    )
    shared = (kinds[0], scales[0], wet_rows, field_tables)
    image, jacobi = operate(2 * columns, window, wet, *shared, True)
    window, wet, residual_dir, known = exchange_second(
        vec_modes, vec_prev, image, jacobi, wet_rows, wet_counts, weights
    )
    (image_r,) = operate(columns, window, wet, *shared, False)
    packed = gram_everywhere(vec_modes, vec_prev, residual_dir, image, image_r, known)
    ndof = 2.0 * lax.axis_size("dom") * wide
    return finish(packed.reshape(LANES, LANES), vec_modes, residual_dir, vec_prev, ndof)


def solution(mesh):
    return jax.shard_map(
        shards,
        mesh=mesh,
        in_specs=(
            P("field", None, "dom"),
            P("field", None, "dom"),
            P("field", None, None),
            P("field", None, None),
            P("field", None, None, None, None),
            P("field", "dom"),
            P("dom"),
            P("dom"),
        ),
        out_specs=(P("field", None, "dom"), P()),
        check_vma=False,
    )
```

```python
import functools

import jax
import jax.numpy as jnp
from jax import lax
from jax.experimental import pallas as pl
from jax.experimental.pallas import tpu as pltpu
from jax.sharding import PartitionSpec as P

BS = 512
LANES = 128
GROUP = 4
UNROLL = 64
PARTS = 4
SPAN = 2048
MESH = pl.DeviceIdType.MESH
NN = (((1,), (0,)), ((), ()))
NT = (((1,), (1,)), ((), ()))


SUB = 8


def split_dot(left, right, dims):
    lh = left.astype(jnp.bfloat16)
    ll = (left - lh.astype(jnp.float32)).astype(jnp.bfloat16)
    rh = right.astype(jnp.bfloat16)
    rl = (right - rh.astype(jnp.float32)).astype(jnp.bfloat16)

    def dot(a, b):
        return lax.dot_general(a, b, dims, preferred_element_type=jnp.float32)

    return dot(lh, rh) + (dot(lh, rl) + dot(ll, rh))


def eliminate(gram, size, inverse_ref):
    panels = size // SUB
    sub = lax.broadcasted_iota(jnp.int32, (SUB, LANES), 0)
    lane = lax.broadcasted_iota(jnp.int32, (SUB, LANES), 1)
    left = [gram[SUB * i : SUB * (i + 1)] for i in range(panels)]
    right = [(lane == sub + SUB * i).astype(jnp.float32) for i in range(panels)]

    def over_lanes(cell, column):
        return jnp.broadcast_to(cell[:, column : column + 1], (SUB, LANES))

    def over_rows(cell, row):
        return jnp.broadcast_to(cell[row : row + 1], (SUB, LANES))

    for k in range(panels):
        columns = [over_lanes(left[k], SUB * k + c) for c in range(SUB)]
        cells = [left[k], right[k]]
        for c in range(SUB):
            pivot = over_rows(columns[c], c)
            root = lax.rsqrt(pivot)
            inverse = root * root
            inverse_ref[SUB * k + c : SUB * k + c + 1] = (cells[1] * root)[c : c + 1]
            here = sub == c
            factor = columns[c]

            def reduced(cell):
                row = over_rows(cell, c) * inverse
                return jnp.where(here, row, cell - factor * row)

            for later in range(c + 1, SUB):
                columns[later] = reduced(columns[later])
            cells = [reduced(cell) for cell in cells]
        rows = [[over_rows(cell, c) for c in range(SUB)] for cell in cells]
        for i in range(k + 1, panels):
            source = left[i]
            for c in range(SUB):
                factor = over_lanes(source, SUB * k + c)
                left[i] = left[i] - factor * rows[0][c]
                right[i] = right[i] - factor * rows[1][c]


def finish_kernel(chunk, scale, packed_ref, x_ref, r_ref, p_ref, basis_ref, projected_ref, inverse_ref, held, sems):
    columns, wide = x_ref.shape
    size = 3 * columns
    packed = packed_ref[...] * scale
    row = lax.broadcasted_iota(jnp.int32, packed.shape, 0)
    col = lax.broadcasted_iota(jnp.int32, packed.shape, 1)
    gram_b = jnp.where(col <= row, packed, packed.T)
    inverse_ref[...] = jnp.zeros_like(inverse_ref)
    eliminate(gram_b, size, inverse_ref)
    high = jnp.concatenate([packed[:, 1:], packed[:, :1]], axis=1)
    gram_a = jnp.where(col >= row, high, high.T)
    gram_a = jnp.where(jnp.maximum(row, col) < size, 0.5 * gram_a, 0.0)
    inverse = inverse_ref[...]
    projected = split_dot(split_dot(inverse, gram_a, NN), inverse, NT)
    projected_ref[...] = projected[:size, :size]
    ih = inverse.astype(jnp.bfloat16)
    il = (inverse - ih.astype(jnp.float32)).astype(jnp.bfloat16)
    twice = jnp.concatenate([ih, ih], axis=1)
    blank = jnp.zeros((LANES - size, chunk), jnp.float32)

    def copy(n):
        span = pl.ds(pl.multiple_of(n * chunk, chunk), chunk)
        return pltpu.make_async_copy(held.at[n], basis_ref.at[0, :, span], sems.at[n])

    def step(n, carry):
        span = pl.ds(pl.multiple_of(n * chunk, chunk), chunk)
        search = jnp.concatenate([x_ref[:, span], r_ref[:, span], p_ref[:, span], blank], axis=0)
        sh = search.astype(jnp.bfloat16)
        sl = (search - sh.astype(jnp.float32)).astype(jnp.bfloat16)
        both = jnp.concatenate([sh, sl], axis=0)
        out = lax.dot_general(twice, both, NN, preferred_element_type=jnp.float32)
        out = out + lax.dot_general(il, sh, NN, preferred_element_type=jnp.float32)
        held[n] = out[:size]
        copy(n).start()
        return carry

    lax.fori_loop(0, wide // chunk, step, 0, unroll=2)

    def close(n, carry):
        copy(n).wait()
        return carry

    lax.fori_loop(0, wide // chunk, close, 0)


def finish(packed, vec_modes, residual_dir, vec_prev, ndof):
    columns, wide = vec_modes.shape
    size = 3 * columns
    chunk = min(512, wide)
    vmem = pl.BlockSpec(memory_space=pltpu.VMEM)
    return pl.pallas_call(
        functools.partial(finish_kernel, chunk, 1.0 / ndof),
        out_shape=(
            jax.ShapeDtypeStruct((1, size, wide), jnp.float32),
            jax.ShapeDtypeStruct((size, size), jnp.float32),
        ),
        in_specs=[vmem, vmem, vmem, vmem],
        out_specs=(pl.BlockSpec(memory_space=pl.ANY), vmem),
        scratch_shapes=[
            pltpu.VMEM((LANES, LANES), jnp.float32),
            pltpu.VMEM((wide // chunk, size, chunk), jnp.float32),
            pltpu.SemaphoreType.DMA((wide // chunk,)),
        ],
        cost_estimate=pl.CostEstimate(
            flops=6 * size * size * wide, bytes_accessed=8 * size * wide, transcendentals=0
        ),
        compiler_params=pltpu.CompilerParams(vmem_limit_bytes=24 * 1024 * 1024),
    )(packed, vec_modes, residual_dir, vec_prev)


def remote(source, target, sems, peer):
    return pltpu.make_async_remote_copy(
        src_ref=source,
        dst_ref=target,
        send_sem=sems[0],
        recv_sem=sems[1],
        device_id=peer,
        device_id_type=MESH,
    )


def greet(peers):
    barrier = pltpu.get_barrier_semaphore()
    for peer in peers:
        pl.semaphore_signal(barrier, inc=1, device_id=peer, device_id_type=MESH)


def greet_ends(field, dom, ends):
    barrier = pltpu.get_barrier_semaphore()

    @pl.when(dom > 0)
    def _():
        pl.semaphore_signal(barrier, inc=1, device_id=(field, dom - 1), device_id_type=MESH)

    @pl.when(dom < ends)
    def _():
        pl.semaphore_signal(barrier, inc=1, device_id=(field, dom + 1), device_id_type=MESH)


def meet(dom, ends, count):
    left = (dom + ends - 1) // ends
    right = (2 * ends - dom - 1) // ends
    pl.semaphore_wait(pltpu.get_barrier_semaphore(), count + left + right)


def clear_ends(window, nbr):
    empty = jnp.zeros((2,) + window.shape[1:], window.dtype)
    window[:2] = empty
    window[nbr + 2 : nbr + 4] = empty


def halo_copies(window, nbr, sems, field, dom):
    send, recv = sems
    left = remote(
        window.at[pl.ds(2, 2)], window.at[pl.ds(nbr + 2, 2)], (send.at[0], recv.at[0]), (field, dom - 1)
    )
    right = remote(
        window.at[pl.ds(nbr, 2)], window.at[pl.ds(0, 2)], (send.at[1], recv.at[1]), (field, dom + 1)
    )
    return left, right


def start_halos(copies, dom, ends):
    left, right = copies

    @pl.when(dom > 0)
    def _():
        left.start()

    @pl.when(dom < ends)
    def _():
        right.start()


def finish_halos(copies, dom, ends):
    left, right = copies

    @pl.when(dom > 0)
    def _():
        left.wait_send()
        right.wait_recv()

    @pl.when(dom < ends)
    def _():
        right.wait_send()
        left.wait_recv()


def pick_rows(read, columns, wide, rows, rows_in, picked):
    slots = picked.shape[0]
    blank = jnp.zeros((LANES - columns, LANES), jnp.float32)

    def turn_in(tile, carry):
        span = pl.ds(pl.multiple_of(tile * LANES, LANES), LANES)
        rows_in[span, :] = jnp.concatenate([read(span), blank], axis=0).T
        return carry

    lax.fori_loop(0, wide // LANES, turn_in, 0, unroll=16)

    def gather(i, carry):
        for slot in range(UNROLL):
            at = i * UNROLL + slot
            picked[pl.ds(at, 1), :] = rows_in[pl.ds(rows[0, at], 1), :]
        return carry

    lax.fori_loop(0, slots // UNROLL, gather, 0)


def send_wet(combine, count, coupling, picked, outgoing, wet, sems, peer):
    slots = picked.shape[0]

    def weigh(i, carry):
        span = pl.ds(pl.multiple_of(i * LANES, LANES), LANES)
        used = i * LANES + lax.broadcasted_iota(jnp.int32, (1, LANES), 1) < count
        weights = jnp.where(used, coupling[pl.ds(i, 1), :], 0.0)
        spread = jnp.broadcast_to(weights, (LANES, LANES)).T
        outgoing[span, :] = (combine(picked[span, :]) * spread).astype(jnp.bfloat16)
        return carry

    cells = slots // LANES
    copies = []
    for part in range(PARTS):
        low, high = cells * part // PARTS, cells * (part + 1) // PARTS
        lax.fori_loop(low, high, weigh, 0, unroll=2)
        span = pl.ds(low * LANES, (high - low) * LANES)
        copy = remote(outgoing.at[span], wet.at[span], (sems[0].at[part], sems[1].at[part]), peer)
        copy.start()
        copies.append(copy)
    return copies


def first_kernel(
    counts, rows_in_hbm, coupling_in, x_in, p_in, tables_in, window, wet, x_ref, p_ref, tables, coupling,
    rows_in, picked, outgoing, side_send, side_recv, end_send, end_recv, rows, loads,
):
    field = lax.axis_index("field")
    dom = lax.axis_index("dom")
    ends = lax.axis_size("dom") - 1
    columns, wide = x_ref.shape
    nbr = wide // BS
    pairs = [(x_in.at[0], x_ref), (p_in.at[0], p_ref), (rows_in_hbm, rows), (coupling_in, coupling), (tables_in.at[0], tables)]
    arrivals = [pltpu.make_async_copy(source, target, loads.at[n]) for n, (source, target) in enumerate(pairs)]
    for arrival in arrivals:
        arrival.start()
    clear_ends(window, nbr)
    greet([(1 - field, dom)])
    greet_ends(field, dom, ends)

    def read(span):
        return jnp.concatenate([x_ref[:, span], p_ref[:, span]], axis=0)

    def fill(n, carry):
        span = pl.ds(pl.multiple_of(n * BS, BS), BS)
        window[n + 2] = read(span).astype(jnp.bfloat16)
        return carry

    arrivals[0].wait()
    arrivals[1].wait()
    lax.fori_loop(0, nbr, fill, 0, unroll=2)
    meet(dom, ends, 1)
    halos = halo_copies(window, nbr, (end_send, end_recv), field, dom)
    start_halos(halos, dom, ends)
    arrivals[2].wait()
    arrivals[3].wait()
    pick_rows(read, 2 * columns, wide, rows, rows_in, picked)
    copies = send_wet(
        lambda cell: cell, counts[0], coupling, picked, outgoing, wet, (side_send, side_recv), (1 - field, dom)
    )
    arrivals[4].wait()
    finish_halos(halos, dom, ends)
    for copy in copies:
        copy.wait()


def exchange_scratch(wide, slots):
    return [
        pltpu.VMEM((wide, LANES), jnp.float32),
        pltpu.VMEM((slots, LANES), jnp.float32),
        pltpu.VMEM((slots, LANES), jnp.bfloat16),
        pltpu.SemaphoreType.DMA((PARTS,)),
        pltpu.SemaphoreType.DMA((PARTS,)),
        pltpu.SemaphoreType.DMA((2,)),
        pltpu.SemaphoreType.DMA((2,)),
    ]


def rows_deep(columns):
    return -(-columns // 16) * 16


SMEM = pl.BlockSpec(memory_space=pltpu.SMEM)
VMEM = pl.BlockSpec(memory_space=pltpu.VMEM)
HBM = pl.BlockSpec(memory_space=pltpu.HBM)


def exchange_first(modes, previous, wet_rows, wet_counts, coupling, tables):
    _, columns, wide = modes.shape
    slots = wet_rows.shape[1]
    held = jax.ShapeDtypeStruct((columns, wide), jnp.float32)
    return pl.pallas_call(
        first_kernel,
        out_shape=(
            jax.ShapeDtypeStruct((wide // BS + 5, rows_deep(2 * columns), BS), jnp.bfloat16),
            jax.ShapeDtypeStruct((slots, LANES), jnp.bfloat16),
            held,
            held,
            jax.ShapeDtypeStruct(tables.shape[1:], tables.dtype),
            jax.ShapeDtypeStruct(coupling.shape, coupling.dtype),
        ),
        in_specs=[SMEM, HBM, HBM, HBM, HBM, HBM],
        out_specs=(VMEM,) * 6,
        scratch_shapes=exchange_scratch(wide, slots)
        + [pltpu.SMEM(wet_rows.shape, jnp.int32), pltpu.SemaphoreType.DMA((5,))],
        compiler_params=pltpu.CompilerParams(
            collective_id=1, has_side_effects=True, vmem_limit_bytes=24 * 1024 * 1024
        ),
    )(wet_counts, wet_rows, coupling, modes, previous, tables)


def gram_over(wide, read, count, out):
    out[...] = jnp.zeros_like(out)

    def add(n, carry):
        span = pl.ds(pl.multiple_of(n * SPAN, SPAN), SPAN)
        left, right = read(span)
        rh = right.astype(jnp.bfloat16)
        rl = (right - rh.astype(jnp.float32)).astype(jnp.bfloat16)
        if left is None:
            lh, ll = rh[:count], rl[:count]
        else:
            lh = left.astype(jnp.bfloat16)
            ll = (left - lh.astype(jnp.float32)).astype(jnp.bfloat16)
        both = lax.dot_general(
            jnp.concatenate([lh, ll], axis=0), rh, NT, preferred_element_type=jnp.float32
        )
        cross = lax.dot_general(lh, rl, NT, preferred_element_type=jnp.float32)
        out[...] += both[:count] + (both[count:] + cross)
        return carry

    lax.fori_loop(0, wide // SPAN, add, 0)


def neighbours(rounds, field, dom):
    groups = []
    for turn, (step, members) in enumerate(rounds):
        low = (1 - 2 * ((dom // step) % 2)) * step
        high = (1 - 2 * ((dom // (2 * step)) % 2)) * 2 * step
        group = [(field, dom + (e % 2) * low + (e // 2) * high) for e in range(members)]
        across = [(1 - field, there) for _, there in group] if turn == 0 else []
        groups.append(group[1:] + across)
    return groups


def gathered(total, landed, members):
    def fold(parts):
        if len(parts) == 4:
            return (parts[0] + parts[1]) + (parts[2] + parts[3])
        return parts[0] + parts[1]

    parts = [total] + landed
    total = fold(parts[:members])
    return total + fold(parts[members:]) if len(parts) > members else total


def sum_rounds():
    bits = (lax.axis_size("dom") - 1).bit_length()
    return [(1 << bit, 4 if bit + 1 < bits else 2) for bit in range(0, bits, 2)]


def second_kernel(
    rounds, counts, rows_hbm, coupling, x_ref, p_ref, image, jacobi, window, wet, r_ref, gram,
    rows_in, picked, outgoing, side_send, side_recv, end_send, end_recv,
    rows, loads, held, landed, sum_send, sum_recv,
):
    field = lax.axis_index("field")
    dom = lax.axis_index("dom")
    ends = lax.axis_size("dom") - 1
    columns, wide = x_ref.shape
    nbr = wide // BS
    deep = window.shape[1]
    arrival = pltpu.make_async_copy(rows_hbm, rows, loads.at[0])
    arrival.start()
    groups = neighbours(rounds, field, dom)
    clear_ends(window, nbr)
    peers = [peer for group in groups for peer in group]
    greet(peers)
    greet_ends(field, dom, ends)

    def add(n, carry):
        span = pl.ds(pl.multiple_of(n * LANES, LANES), LANES)
        x = x_ref[:, span]
        return carry[0] + x * x, carry[1] + x * image[:columns, span]

    zero = jnp.zeros((columns, LANES), jnp.float32)
    squares, products = lax.fori_loop(0, wide // LANES, add, (zero, zero), unroll=8)
    lane = lax.broadcasted_iota(jnp.int32, (columns, LANES), 1)
    total = jnp.where(
        lane == 0,
        jnp.sum(squares, axis=1, keepdims=True),
        jnp.where(lane == 1, jnp.sum(products, axis=1, keepdims=True), 0.0),
    )
    total = jnp.concatenate([total, jnp.zeros((LANES - columns, LANES), jnp.float32)], axis=0).T[:SUB]
    arrival.wait()
    meet(dom, ends, len(peers))
    for turn, group in enumerate(groups):
        held[turn] = total
        copies = [
            remote(held.at[turn], landed.at[turn, e], (sum_send.at[turn, e], sum_recv.at[turn, e]), peer)
            for e, peer in enumerate(group)
        ]
        for copy in copies:
            copy.start()
        if turn == 0:
            pick_rows(
                lambda span: jnp.concatenate(
                    [image[:columns, span] / jacobi[:, span], x_ref[:, span] / jacobi[:, span]], axis=0
                ),
                2 * columns, wide, rows, rows_in, picked,
            )
        for copy in copies:
            copy.wait()
        members = rounds[turn][1]
        total = gathered(total, [landed[turn, e] for e in range(len(group))], members)
    lane = lax.broadcasted_iota(jnp.int32, (1, LANES), 1)
    across = jnp.where(lane < columns, total[1:2] / total[0:1], 0.0)
    total = jnp.concatenate([total, jnp.zeros((LANES - SUB, LANES), jnp.float32)], axis=0).T[:columns]
    quotient = total[:, 1:2] / total[:, 0:1]
    extra = jnp.zeros((deep - columns, BS), jnp.float32)

    def fill(n, carry):
        span = pl.ds(pl.multiple_of(n * BS, BS), BS)
        r = (image[:columns, span] - x_ref[:, span] * quotient) / jacobi[:, span]
        r_ref[:, span] = r
        window[n + 2] = jnp.concatenate([r, extra], axis=0).astype(jnp.bfloat16)
        return carry

    for n in (0, 1, nbr - 2, nbr - 1):
        fill(n, 0)
    halos = halo_copies(window, nbr, (end_send, end_recv), field, dom)
    start_halos(halos, dom, ends)
    copies = send_wet(
        lambda cell: cell - pltpu.roll(cell, LANES - columns, 1) * across,
        counts[0], coupling, picked, outgoing, wet, (side_send, side_recv), (1 - field, dom),
    )
    lax.fori_loop(2, nbr - 2, fill, 0)
    spare = jnp.zeros((gram.shape[1] - 5 * columns, SPAN), jnp.float32)
    gram_over(
        wide,
        lambda span: (
            None,
            jnp.concatenate([x_ref[:, span], p_ref[:, span], r_ref[:, span], image[:, span], spare], axis=0),
        ),
        gram.shape[0],
        gram,
    )
    finish_halos(halos, dom, ends)
    for copy in copies:
        copy.wait()


def exchange_second(vec_modes, vec_prev, image, jacobi, wet_rows, wet_counts, coupling):
    columns, wide = vec_modes.shape
    slots = wet_rows.shape[1]
    rounds = sum_rounds()
    most = 2 * rounds[0][1] - 1
    return pl.pallas_call(
        functools.partial(second_kernel, rounds),
        out_shape=(
            jax.ShapeDtypeStruct((wide // BS + 5, rows_deep(columns), BS), jnp.bfloat16),
            jax.ShapeDtypeStruct((slots, LANES), jnp.bfloat16),
            jax.ShapeDtypeStruct((columns, wide), jnp.float32),
            jax.ShapeDtypeStruct((LANES, rows_deep(5 * columns)), jnp.float32),
        ),
        in_specs=[SMEM, HBM, VMEM, VMEM, VMEM, VMEM, VMEM],
        out_specs=(VMEM,) * 4,
        scratch_shapes=exchange_scratch(wide, slots)
        + [
            pltpu.SMEM(wet_rows.shape, jnp.int32),
            pltpu.SemaphoreType.DMA((1,)),
            pltpu.VMEM((len(rounds), SUB, LANES), jnp.float32),
            pltpu.VMEM((len(rounds), most, SUB, LANES), jnp.float32),
            pltpu.SemaphoreType.DMA((len(rounds), most)),
            pltpu.SemaphoreType.DMA((len(rounds), most)),
        ],
        compiler_params=pltpu.CompilerParams(
            collective_id=3, has_side_effects=True, vmem_limit_bytes=20 * 1024 * 1024
        ),
    )(wet_counts, wet_rows, coupling, vec_modes, vec_prev, image, jacobi)


def gram_kernel(
    rounds, x_ref, p_ref, r_ref, image_r, known, o_ref,
    fresh, gram_b, gram_a, packed, held, landed, across, send_sem, recv_sem, side_send, side_recv,
):
    field = lax.axis_index("field")
    dom = lax.axis_index("dom")
    columns, wide = x_ref.shape
    groups = []
    for step, members in rounds:
        low = (1 - 2 * ((dom // step) % 2)) * step
        high = (1 - 2 * ((dom // (2 * step)) % 2)) * 2 * step
        groups.append([dom + (e % 2) * low + (e // 2) * high for e in range(1, members)])
    peers = [(1 - field, dom)] + [(field, peer) for group in groups for peer in group]
    greet(peers)
    n = columns
    low = jnp.zeros((fresh.shape[0] - n, SPAN), jnp.float32)
    spare = jnp.zeros((LANES - 3 * n, SPAN), jnp.float32)
    gram_over(
        wide,
        lambda span: (
            jnp.concatenate([image_r[:, span], low], axis=0),
            jnp.concatenate([x_ref[:, span], p_ref[:, span], r_ref[:, span], spare], axis=0),
        ),
        fresh.shape[0],
        fresh,
    )
    old = known[...]
    turned = jnp.concatenate(
        [fresh[...], jnp.zeros((LANES - fresh.shape[0], LANES), jnp.float32)], axis=0
    ).T
    gram_b[...] = jnp.zeros_like(gram_b)
    gram_a[...] = jnp.zeros_like(gram_a)
    x, r, p = slice(0, n), slice(n, 2 * n), slice(2 * n, 3 * n)
    kx, kp, kr = slice(0, n), slice(n, 2 * n), slice(2 * n, 3 * n)
    ax, ap = slice(3 * n, 4 * n), slice(4 * n, 5 * n)
    for rows, here in ((x, kx), (r, kr), (p, kp)):
        gram_a[rows, x] = old[here, ax]
        gram_a[rows, r] = turned[here, :n]
        gram_a[rows, p] = old[here, ap]
    for rows, here, cols, there in (
        (x, kx, x, kx), (r, kr, x, kx), (r, kr, r, kr), (p, kp, x, kx), (p, kp, r, kr), (p, kp, p, kp),
    ):
        gram_b[rows, cols] = old[here, there]
    both = gram_a[...] + gram_a[...].T
    both = jnp.concatenate([both[:, LANES - 1 :], both[:, : LANES - 1]], axis=1)
    row = lax.broadcasted_iota(jnp.int32, (LANES, LANES), 0)
    col = lax.broadcasted_iota(jnp.int32, (LANES, LANES), 1)
    half = LANES // 2
    whole = jnp.where(col <= row, gram_b[...], both)
    packed[0] = whole[:half]
    packed[1] = whole[half:]
    pl.semaphore_wait(pltpu.get_barrier_semaphore(), len(peers))
    copy = remote(packed.at[1 - field], across.at[0], (side_send.at[0], side_recv.at[0]), (1 - field, dom))
    copy.start()
    copy.wait()
    total = packed[field] + across[0]
    for turn, group in enumerate(groups):
        held[turn] = total
        copies = [
            remote(
                held.at[turn], landed.at[turn, e], (send_sem.at[turn, e], recv_sem.at[turn, e]), (field, peer)
            )
            for e, peer in enumerate(group)
        ]
        for copy in copies:
            copy.start()
        for copy in copies:
            copy.wait()
        total = gathered(total, [landed[turn, e] for e in range(len(group))], rounds[turn][1])
    o_ref[field] = total
    held[len(groups)] = total
    copy = remote(held.at[len(groups)], across.at[1], (side_send.at[1], side_recv.at[1]), (1 - field, dom))
    copy.start()
    copy.wait()
    o_ref[1 - field] = across[1]


def gram_everywhere(vec_modes, vec_prev, residual_dir, image_r, known):
    columns = vec_modes.shape[0]
    rounds = sum_rounds()
    slots = len(rounds)
    cell = (LANES // 2, LANES)
    return pl.pallas_call(
        functools.partial(gram_kernel, rounds),
        out_shape=jax.ShapeDtypeStruct((2,) + cell, jnp.float32),
        in_specs=[VMEM] * 5,
        out_specs=VMEM,
        scratch_shapes=[
            pltpu.VMEM((rows_deep(columns), LANES), jnp.float32),
            pltpu.VMEM((LANES, LANES), jnp.float32),
            pltpu.VMEM((LANES, LANES), jnp.float32),
            pltpu.VMEM((2,) + cell, jnp.float32),
            pltpu.VMEM((slots + 1,) + cell, jnp.float32),
            pltpu.VMEM((slots, 3) + cell, jnp.float32),
            pltpu.VMEM((2,) + cell, jnp.float32),
            pltpu.SemaphoreType.DMA((slots, 3)),
            pltpu.SemaphoreType.DMA((slots, 3)),
            pltpu.SemaphoreType.DMA((2,)),
            pltpu.SemaphoreType.DMA((2,)),
        ],
        compiler_params=pltpu.CompilerParams(
            collective_id=2, has_side_effects=True, vmem_limit_bytes=16 * 1024 * 1024
        ),
    )(vec_modes, vec_prev, residual_dir, image_r, known)


def group_rows(kind_of, lists, nbr, types, cells):
    spare = nbr + 2
    bits = 32 // types
    mask = (1 << bits) - 1
    for offset in range(3):
        for slot in range(cells * GROUP):
            lists[offset, slot] = spare
        first = 2 - offset
        shifts = [kind_of(offset, row) * bits for row in range(first, nbr + 2)]
        count = jnp.int32(0)
        ranks = []
        for shift in shifts:
            ranks.append(lax.shift_right_logical(count, shift) & mask)
            count = count + lax.shift_left(jnp.int32(1), shift)
        starts = jnp.int32(0)
        place = jnp.int32(0)
        for kind in range(types):
            starts = starts + place * (1 << bits * kind)
            here = lax.shift_right_logical(count, jnp.int32(bits * kind)) & mask
            place = place + ((here + (GROUP - 1)) & -GROUP)
        for n, (shift, rank) in enumerate(zip(shifts, ranks)):
            lists[offset, (lax.shift_right_logical(starts, shift) & mask) + rank] = n + first


def operator_kernel(cells, with_diagonal, kinds, scales, rows_hbm, window, wet, tables, o_ref, *rest):
    if with_diagonal:
        jacobi, diagonal, total, rows_in, rows_out, lists, rows, loads = rest
    else:
        total, rows_in, rows_out, lists, rows, loads = rest
    columns, wide = o_ref.shape
    nbr = wide // BS
    types = tables.shape[1]
    deep = window.shape[1]
    slots = wet.shape[0]
    arrival = pltpu.make_async_copy(rows_hbm, rows, loads.at[0])
    arrival.start()
    base = lax.axis_index("dom") * nbr - 2
    every = kinds.shape[0] // 3

    def kind_of(offset, row):
        return kinds[offset * every + jnp.maximum(base + row, 0)]

    def scale_of(offset, row):
        return scales[offset * every + jnp.maximum(base + row, 0)]

    group_rows(kind_of, lists, nbr, types, cells)

    def clear(n, carry):
        total[n] = jnp.zeros(total.shape[1:], jnp.float32)
        span = pl.ds(pl.multiple_of(n * BS, BS), BS)
        rows_out[span, :] = jnp.zeros((BS, LANES), jnp.float32)
        return carry

    lax.fori_loop(0, nbr, clear, 0)

    def widen(i, carry):
        span = pl.ds(pl.multiple_of(i * LANES, LANES), LANES)
        rows_in[span, :] = wet[span, :].astype(jnp.float32)
        return carry

    lax.fori_loop(0, slots // LANES, widen, 0, unroll=4)
    arrival.wait()

    def scatter(i, carry):
        for slot in range(UNROLL):
            at = i * UNROLL + slot
            rows_out[pl.ds(rows[0, at], 1), :] = rows_in[pl.ds(at, 1), :]
        return carry

    lax.fori_loop(0, slots // UNROLL, scatter, 0)
    if with_diagonal:
        eye = lax.broadcasted_iota(jnp.int32, (LANES, LANES), 0) == lax.broadcasted_iota(
            jnp.int32, (LANES, LANES), 1
        )
        for kind in range(types):
            for part in range(BS // LANES):
                span = slice(part * LANES, (part + 1) * LANES)
                cell = tables[0, kind, span, span].astype(jnp.float32)
                diagonal[kind, :, span] = jnp.sum(jnp.where(eye, cell, 0.0), axis=0, keepdims=True)
        for n in range(nbr):
            jacobi[:, n * BS : (n + 1) * BS] = scale_of(0, n + 2) * diagonal[kind_of(0, n + 2)]

    def step(i, carry):
        for offset in range(3):
            found = [lists[offset, i * GROUP + u] for u in range(GROUP)]
            held = [jnp.minimum(row, nbr + 1) for row in found]
            kind = kind_of(offset, held[0])
            factors = [scale_of(offset, row) for row in held]
            for ahead in (True, False) if offset else (True,):
                if ahead:
                    sources = [row + offset for row in found]
                    targets = [jnp.where(row < 2, nbr, row - 2) for row in found]
                else:
                    sources = found
                    targets = [jnp.minimum(row - 2 + offset, nbr) for row in found]
                left = jnp.concatenate([window[source] for source in sources], axis=0)
                product = lax.dot_general(
                    left,
                    tables[offset, kind],
                    NT if ahead and offset else NN,
                    preferred_element_type=jnp.float32,
                )
                for u in range(GROUP):
                    total[targets[u]] += factors[u] * product[u * deep : (u + 1) * deep]
        return carry

    lax.fori_loop(0, cells, step, 0)
    parts = BS // LANES

    def turn_out(n, carry):
        for part in range(parts):
            span = pl.ds(pl.multiple_of(n * BS + part * LANES, LANES), LANES)
            inner = slice(part * LANES, (part + 1) * LANES)
            o_ref[:, span] = total[n, :columns, inner] + rows_out[span, :].T[:columns]
        return carry

    lax.fori_loop(0, nbr, turn_out, 0, unroll=4)


def operate(columns, window, wet, kinds, scales, rows, tables, with_diagonal):
    nbr = window.shape[0] - 5
    wide = nbr * BS
    deep = window.shape[1]
    slots = wet.shape[0]
    types = tables.shape[1]
    cells = (nbr + 2 + types * (GROUP - 1)) // GROUP
    outs = [jax.ShapeDtypeStruct((columns, wide), jnp.float32)]
    scratch = [
        pltpu.VMEM((nbr + 1, deep, BS), jnp.float32),
        pltpu.VMEM((slots, LANES), jnp.float32),
        pltpu.VMEM((wide, LANES), jnp.float32),
        pltpu.SMEM((3, cells * GROUP), jnp.int32),
        pltpu.SMEM(rows.shape, jnp.int32),
        pltpu.SemaphoreType.DMA((1,)),
    ]
    if with_diagonal:
        outs.append(jax.ShapeDtypeStruct((1, wide), jnp.float32))
        scratch = [pltpu.VMEM((types, 1, BS), jnp.float32)] + scratch
    return pl.pallas_call(
        functools.partial(operator_kernel, cells, with_diagonal),
        out_shape=tuple(outs),
        in_specs=[SMEM, SMEM, HBM, VMEM, VMEM, VMEM],
        out_specs=(VMEM,) * len(outs),
        scratch_shapes=scratch,
        cost_estimate=pl.CostEstimate(
            flops=10 * columns * wide * BS, bytes_accessed=16 * columns * wide, transcendentals=0
        ),
        compiler_params=pltpu.CompilerParams(vmem_limit_bytes=24 * 1024 * 1024),
    )(kinds, scales, rows, window, wet, tables)


def shards(modes, previous, kinds, scales, tables, wet_rows, wet_counts, coupling):
    modes, previous, tables, wet_rows, coupling = [
        pltpu.with_memory_space_constraint(a, pltpu.HBM) for a in (modes, previous, tables, wet_rows, coupling.reshape(-1, LANES))
    ]
    _, columns, wide = modes.shape
    window, wet, vec_modes, vec_prev, field_tables, weights = exchange_first(
        modes, previous, wet_rows, wet_counts, coupling, tables
    )
    shared = (kinds.reshape(-1), scales.reshape(-1), wet_rows, field_tables)
    image, jacobi = operate(2 * columns, window, wet, *shared, True)
    window, wet, residual_dir, known = exchange_second(
        vec_modes, vec_prev, image, jacobi, wet_rows, wet_counts, weights
    )
    (image_r,) = operate(columns, window, wet, *shared, False)
    packed = gram_everywhere(vec_modes, vec_prev, residual_dir, image_r, known)
    ndof = 2.0 * lax.axis_size("dom") * wide
    return finish(packed.reshape(LANES, LANES), vec_modes, residual_dir, vec_prev, ndof)


def solution(mesh):
    return jax.shard_map(
        shards,
        mesh=mesh,
        in_specs=(
            P("field", None, "dom"),
            P("field", None, "dom"),
            P("field", None, None),
            P("field", None, None),
            P("field", None, None, None, None),
            P("field", "dom"),
            P("dom"),
            P("dom"),
        ),
        out_specs=(P("field", None, "dom"), P()),
        check_vma=False,
    )
```

```python
import functools

import jax
import jax.numpy as jnp
from jax import lax
from jax.experimental import pallas as pl
from jax.experimental.pallas import tpu as pltpu
from jax.sharding import PartitionSpec as P

BS = 512
LANES = 128
GROUP = 4
GROUP_WIDE = 3
PARTS = 4
SPAN = 2048
MESH = pl.DeviceIdType.MESH
NN = (((1,), (0,)), ((), ()))
NT = (((1,), (1,)), ((), ()))


SUB = 8


def split_dot(left, right, dims):
    lh = left.astype(jnp.bfloat16)
    ll = (left - lh.astype(jnp.float32)).astype(jnp.bfloat16)
    rh = right.astype(jnp.bfloat16)
    rl = (right - rh.astype(jnp.float32)).astype(jnp.bfloat16)

    def dot(a, b):
        return lax.dot_general(a, b, dims, preferred_element_type=jnp.float32)

    return dot(lh, rh) + (dot(lh, rl) + dot(ll, rh))


def eliminate(gram, size, inverse_ref):
    panels = size // SUB
    sub = lax.broadcasted_iota(jnp.int32, (SUB, LANES), 0)
    lane = lax.broadcasted_iota(jnp.int32, (SUB, LANES), 1)
    left = [gram[SUB * i : SUB * (i + 1)] for i in range(panels)]
    right = [(lane == sub + SUB * i).astype(jnp.float32) for i in range(panels)]

    def over_lanes(cell, column):
        return jnp.broadcast_to(cell[:, column : column + 1], (SUB, LANES))

    def over_rows(cell, row):
        return jnp.broadcast_to(cell[row : row + 1], (SUB, LANES))

    for k in range(panels):
        columns = [over_lanes(left[k], SUB * k + c) for c in range(SUB)]
        cells = [left[k], right[k]]
        for c in range(SUB):
            pivot = over_rows(columns[c], c)
            root = lax.rsqrt(pivot)
            inverse = root * root
            inverse_ref[SUB * k + c : SUB * k + c + 1] = (cells[1] * root)[c : c + 1]
            here = sub == c
            factor = columns[c]

            def reduced(cell):
                row = over_rows(cell, c) * inverse
                return jnp.where(here, row, cell - factor * row)

            for later in range(c + 1, SUB):
                columns[later] = reduced(columns[later])
            cells = [reduced(cell) for cell in cells]
        rows = [[over_rows(cell, c) for c in range(SUB)] for cell in cells]
        for i in range(k + 1, panels):
            source = left[i]
            for c in range(SUB):
                factor = over_lanes(source, SUB * k + c)
                left[i] = left[i] - factor * rows[0][c]
                right[i] = right[i] - factor * rows[1][c]


def finish_kernel(columns, chunk, scale, packed_ref, split, basis_ref, projected_ref, inverse_ref, held, sems):
    wide = split.shape[1]
    size = 3 * columns
    packed = packed_ref[...] * scale
    row = lax.broadcasted_iota(jnp.int32, packed.shape, 0)
    col = lax.broadcasted_iota(jnp.int32, packed.shape, 1)
    gram_b = jnp.where(col <= row, packed, packed.T)
    inverse_ref[...] = jnp.zeros_like(inverse_ref)
    eliminate(gram_b, size, inverse_ref)
    high = jnp.concatenate([packed[:, 1:], packed[:, :1]], axis=1)
    gram_a = jnp.where(col >= row, high, high.T)
    gram_a = jnp.where(jnp.maximum(row, col) < size, 0.5 * gram_a, 0.0)
    inverse = inverse_ref[...]
    projected = split_dot(split_dot(inverse, gram_a, NN), inverse, NT)
    projected_ref[...] = projected[:size, :size]
    inverse = jnp.concatenate(
        [
            inverse[:, :columns],
            inverse[:, 2 * columns : size],
            inverse[:, columns : 2 * columns],
            inverse[:, size:],
        ],
        axis=1,
    )
    ih = inverse.astype(jnp.bfloat16)
    il = (inverse - ih.astype(jnp.float32)).astype(jnp.bfloat16)
    twice = jnp.concatenate([ih, ih], axis=1)

    def copy(n):
        span = pl.ds(pl.multiple_of(n * chunk, chunk), chunk)
        return pltpu.make_async_copy(held.at[n], basis_ref.at[0, :, span], sems.at[n])

    def step(n, carry):
        span = pl.ds(pl.multiple_of(n * chunk, chunk), chunk)
        out = lax.dot_general(twice, split[:, span], NN, preferred_element_type=jnp.float32)
        out = out + lax.dot_general(il, split[:LANES, span], NN, preferred_element_type=jnp.float32)
        held[n] = out[:size]
        copy(n).start()
        return carry

    lax.fori_loop(0, wide // chunk, step, 0, unroll=2)

    def close(n, carry):
        copy(n).wait()
        return carry

    lax.fori_loop(0, wide // chunk, close, 0)


def finish(columns, packed, split, ndof):
    wide = split.shape[1]
    size = 3 * columns
    chunk = min(512, wide)
    vmem = pl.BlockSpec(memory_space=pltpu.VMEM)
    return pl.pallas_call(
        functools.partial(finish_kernel, columns, chunk, 1.0 / ndof),
        out_shape=(
            jax.ShapeDtypeStruct((1, size, wide), jnp.float32),
            jax.ShapeDtypeStruct((size, size), jnp.float32),
        ),
        in_specs=[vmem, vmem],
        out_specs=(pl.BlockSpec(memory_space=pl.ANY), vmem),
        scratch_shapes=[
            pltpu.VMEM((LANES, LANES), jnp.float32),
            pltpu.VMEM((wide // chunk, size, chunk), jnp.float32),
            pltpu.SemaphoreType.DMA((wide // chunk,)),
        ],
        cost_estimate=pl.CostEstimate(
            flops=6 * size * size * wide, bytes_accessed=8 * size * wide, transcendentals=0
        ),
        compiler_params=pltpu.CompilerParams(vmem_limit_bytes=24 * 1024 * 1024),
    )(packed, split)


def remote(source, target, sems, peer):
    return pltpu.make_async_remote_copy(
        src_ref=source,
        dst_ref=target,
        send_sem=sems[0],
        recv_sem=sems[1],
        device_id=peer,
        device_id_type=MESH,
    )


def greet(peers):
    barrier = pltpu.get_barrier_semaphore()
    for peer in peers:
        pl.semaphore_signal(barrier, inc=1, device_id=peer, device_id_type=MESH)


def greet_ends(field, dom, ends):
    barrier = pltpu.get_barrier_semaphore()

    @pl.when(dom > 0)
    def _():
        pl.semaphore_signal(barrier, inc=1, device_id=(field, dom - 1), device_id_type=MESH)

    @pl.when(dom < ends)
    def _():
        pl.semaphore_signal(barrier, inc=1, device_id=(field, dom + 1), device_id_type=MESH)


def meet(dom, ends, count):
    left = (dom + ends - 1) // ends
    right = (2 * ends - dom - 1) // ends
    pl.semaphore_wait(pltpu.get_barrier_semaphore(), count + left + right)


def clear_ends(window, nbr):
    empty = jnp.zeros((2,) + window.shape[1:], window.dtype)
    window[:2] = empty
    window[nbr + 2 : nbr + 4] = empty


def halo_copies(window, nbr, sems, field, dom):
    send, recv = sems
    left = remote(
        window.at[pl.ds(2, 2)], window.at[pl.ds(nbr + 2, 2)], (send.at[0], recv.at[0]), (field, dom - 1)
    )
    right = remote(
        window.at[pl.ds(nbr, 2)], window.at[pl.ds(0, 2)], (send.at[1], recv.at[1]), (field, dom + 1)
    )
    return left, right


def start_halos(copies, dom, ends):
    left, right = copies

    @pl.when(dom > 0)
    def _():
        left.start()

    @pl.when(dom < ends)
    def _():
        right.start()


def finish_halos(copies, dom, ends):
    left, right = copies

    @pl.when(dom > 0)
    def _():
        left.wait_send()
        right.wait_recv()

    @pl.when(dom < ends)
    def _():
        right.wait_send()
        left.wait_recv()


def turn_rows(read, columns, wide, rows_in):
    blank = jnp.zeros((LANES - columns, LANES), jnp.float32)

    def turn_in(tile, carry):
        span = pl.ds(pl.multiple_of(tile * LANES, LANES), LANES)
        rows_in[span, :] = jnp.concatenate([read(span), blank], axis=0).T
        return carry

    lax.fori_loop(0, wide // LANES, turn_in, 0, unroll=16)


def pick_rows(low, high, rows, rows_in, picked):
    def gather(i, carry):
        for slot in range(LANES):
            picked[pl.ds(i * LANES + slot, 1), :] = rows_in[pl.ds(rows[i, slot], 1), :]
        return carry

    lax.fori_loop(low, high, gather, 0)


def spread_weights(count, coupling, spread):
    def one(i, carry):
        span = pl.ds(pl.multiple_of(i * LANES, LANES), LANES)
        used = i * LANES + lax.broadcasted_iota(jnp.int32, (1, LANES), 1) < count
        weights = jnp.where(used, coupling[pl.ds(i, 1), :], 0.0)
        spread[span, :] = jnp.broadcast_to(weights, (LANES, LANES)).T
        return carry

    lax.fori_loop(0, coupling.shape[0], one, 0, unroll=4)


def send_wet(prepare, combine, spread, picked, outgoing, wet, sems, peer):
    cells = picked.shape[0] // LANES

    def weigh(i, carry):
        span = pl.ds(pl.multiple_of(i * LANES, LANES), LANES)
        outgoing[span, :] = (combine(picked[span, :]) * spread[span, :]).astype(jnp.bfloat16)
        return carry

    copies = []
    for part in range(PARTS):
        low, high = cells * part // PARTS, cells * (part + 1) // PARTS
        prepare(low, high)
        lax.fori_loop(low, high, weigh, 0, unroll=2)
        span = pl.ds(low * LANES, (high - low) * LANES)
        copy = remote(outgoing.at[span], wet.at[span], (sems[0].at[part], sems[1].at[part]), peer)
        copy.start()
        copies.append(copy)
    return copies


def first_kernel(
    counts, rows_in_hbm, coupling_in, x_in, p_in, tables_in, window, wet, x_ref, p_ref, tables, coupling,
    rows_in, picked, spread, outgoing, side_send, side_recv, end_send, end_recv, rows, loads,
):
    field = lax.axis_index("field")
    dom = lax.axis_index("dom")
    ends = lax.axis_size("dom") - 1
    columns, wide = x_ref.shape
    nbr = wide // BS
    pairs = [(x_in.at[0], x_ref), (p_in.at[0], p_ref), (rows_in_hbm, rows), (coupling_in, coupling), (tables_in.at[0], tables)]
    arrivals = [pltpu.make_async_copy(source, target, loads.at[n]) for n, (source, target) in enumerate(pairs)]
    for arrival in arrivals[:4]:
        arrival.start()
    clear_ends(window, nbr)
    greet([(1 - field, dom)])
    greet_ends(field, dom, ends)

    def read(span):
        return jnp.concatenate([x_ref[:, span], p_ref[:, span]], axis=0)

    def fill(n, carry):
        span = pl.ds(pl.multiple_of(n * BS, BS), BS)
        window[n + 2] = read(span).astype(jnp.bfloat16)
        return carry

    arrivals[3].wait()
    spread_weights(counts[0], coupling, spread)
    arrivals[0].wait()
    arrivals[1].wait()
    arrivals[4].start()
    lax.fori_loop(0, nbr, fill, 0, unroll=2)
    meet(dom, ends, 1)
    halos = halo_copies(window, nbr, (end_send, end_recv), field, dom)
    start_halos(halos, dom, ends)
    arrivals[2].wait()
    turn_rows(read, 2 * columns, wide, rows_in)
    copies = send_wet(
        lambda low, high: pick_rows(low, high, rows, rows_in, picked),
        lambda cell: cell, spread, picked, outgoing, wet, (side_send, side_recv), (1 - field, dom),
    )
    arrivals[4].wait()
    finish_halos(halos, dom, ends)
    for copy in copies:
        copy.wait()


def exchange_scratch(wide, slots):
    return [
        pltpu.VMEM((wide, LANES), jnp.float32),
        pltpu.VMEM((slots, LANES), jnp.float32),
        pltpu.VMEM((slots, LANES), jnp.float32),
        pltpu.VMEM((slots, LANES), jnp.bfloat16),
        pltpu.SemaphoreType.DMA((PARTS,)),
        pltpu.SemaphoreType.DMA((PARTS,)),
        pltpu.SemaphoreType.DMA((2,)),
        pltpu.SemaphoreType.DMA((2,)),
    ]


def rows_deep(columns):
    return -(-columns // 16) * 16


SMEM = pl.BlockSpec(memory_space=pltpu.SMEM)
VMEM = pl.BlockSpec(memory_space=pltpu.VMEM)
HBM = pl.BlockSpec(memory_space=pltpu.HBM)


def exchange_first(modes, previous, wet_rows, wet_counts, coupling, tables):
    _, columns, wide = modes.shape
    slots = wet_rows.size
    held = jax.ShapeDtypeStruct((columns, wide), jnp.float32)
    return pl.pallas_call(
        first_kernel,
        out_shape=(
            jax.ShapeDtypeStruct((wide // BS + 5, rows_deep(2 * columns), BS), jnp.bfloat16),
            jax.ShapeDtypeStruct((slots, LANES), jnp.bfloat16),
            held,
            held,
            jax.ShapeDtypeStruct(tables.shape[1:], tables.dtype),
            jax.ShapeDtypeStruct(coupling.shape, coupling.dtype),
        ),
        in_specs=[SMEM, HBM, HBM, HBM, HBM, HBM],
        out_specs=(VMEM,) * 6,
        scratch_shapes=exchange_scratch(wide, slots)
        + [pltpu.SMEM(wet_rows.shape, jnp.int32), pltpu.SemaphoreType.DMA((5,))],
        compiler_params=pltpu.CompilerParams(
            collective_id=1, has_side_effects=True, vmem_limit_bytes=24 * 1024 * 1024
        ),
    )(wet_counts, wet_rows, coupling, modes, previous, tables)


def parts_of(cell):
    high = cell.astype(jnp.bfloat16)
    return high, (cell - high.astype(jnp.float32)).astype(jnp.bfloat16)


def gram_over(wide, read, out):
    out[...] = jnp.zeros_like(out)
    count = out.shape[0]

    def add(n, carry):
        span = pl.ds(pl.multiple_of(n * SPAN, SPAN), SPAN)
        (lh, ll), (rh, rl) = read(span)
        both = lax.dot_general(
            jnp.concatenate([lh, ll], axis=0), rh, NT, preferred_element_type=jnp.float32
        )
        cross = lax.dot_general(lh, rl, NT, preferred_element_type=jnp.float32)
        out[...] += both[:count] + (both[count:] + cross)
        return carry

    lax.fori_loop(0, wide // SPAN, add, 0)


def neighbours(rounds, field, dom):
    groups = []
    for turn, (step, members) in enumerate(rounds):
        low = (1 - 2 * ((dom // step) % 2)) * step
        high = (1 - 2 * ((dom // (2 * step)) % 2)) * 2 * step
        group = [(field, dom + (e % 2) * low + (e // 2) * high) for e in range(members)]
        across = [(1 - field, there) for _, there in group] if turn == 0 else []
        groups.append(group[1:] + across)
    return groups


def gathered(total, landed, members):
    def fold(parts):
        if len(parts) == 4:
            return (parts[0] + parts[1]) + (parts[2] + parts[3])
        return parts[0] + parts[1]

    parts = [total] + landed
    total = fold(parts[:members])
    return total + fold(parts[members:]) if len(parts) > members else total


def sum_rounds():
    bits = (lax.axis_size("dom") - 1).bit_length()
    return [(1 << bit, 4 if bit + 1 < bits else 2) for bit in range(0, bits, 2)]


def second_kernel(
    rounds, counts, rows_hbm, coupling, x_ref, p_ref, image, jacobi, window, wet, gram, split,
    rows_in, picked, spread, outgoing, side_send, side_recv, end_send, end_recv,
    rows, loads, held, landed, sum_send, sum_recv, r_ref,
):
    field = lax.axis_index("field")
    dom = lax.axis_index("dom")
    ends = lax.axis_size("dom") - 1
    columns, wide = x_ref.shape
    nbr = wide // BS
    deep = window.shape[1]
    arrival = pltpu.make_async_copy(rows_hbm, rows, loads.at[0])
    arrival.start()
    groups = neighbours(rounds, field, dom)
    clear_ends(window, nbr)
    peers = [peer for group in groups for peer in group]
    greet(peers)
    greet_ends(field, dom, ends)

    def add(n, carry):
        span = pl.ds(pl.multiple_of(n * LANES, LANES), LANES)
        x = x_ref[:, span]
        return carry[0] + x * x, carry[1] + x * image[:columns, span]

    zero = jnp.zeros((columns, LANES), jnp.float32)
    squares, products = lax.fori_loop(0, wide // LANES, add, (zero, zero), unroll=8)
    lane = lax.broadcasted_iota(jnp.int32, (columns, LANES), 1)
    total = jnp.where(
        lane == 0,
        jnp.sum(squares, axis=1, keepdims=True),
        jnp.where(lane == 1, jnp.sum(products, axis=1, keepdims=True), 0.0),
    )
    total = jnp.concatenate([total, jnp.zeros((LANES - columns, LANES), jnp.float32)], axis=0).T[:SUB]
    arrival.wait()
    meet(dom, ends, len(peers))
    for turn, group in enumerate(groups):
        held[turn] = total
        copies = [
            remote(held.at[turn], landed.at[turn, e], (sum_send.at[turn, e], sum_recv.at[turn, e]), peer)
            for e, peer in enumerate(group)
        ]
        for copy in copies:
            copy.start()
        if turn == 0:
            turn_rows(
                lambda span: jnp.concatenate(
                    [image[:columns, span] / jacobi[:, span], x_ref[:, span] / jacobi[:, span]], axis=0
                ),
                2 * columns, wide, rows_in,
            )
        if turn == len(groups) - 1:
            pick_rows(0, rows.shape[0], rows, rows_in, picked)
            spread_weights(counts[0], coupling, spread)
        for copy in copies:
            copy.wait()
        members = rounds[turn][1]
        total = gathered(total, [landed[turn, e] for e in range(len(group))], members)
    lane = lax.broadcasted_iota(jnp.int32, (1, LANES), 1)
    across = jnp.where(lane < columns, total[1:2] / total[0:1], 0.0)
    total = jnp.concatenate([total, jnp.zeros((LANES - SUB, LANES), jnp.float32)], axis=0).T[:columns]
    quotient = total[:, 1:2] / total[:, 0:1]
    extra = jnp.zeros((deep - columns, BS), jnp.float32)

    def fill(n, carry):
        span = pl.ds(pl.multiple_of(n * BS, BS), BS)
        r = (image[:columns, span] - x_ref[:, span] * quotient) / jacobi[:, span]
        r_ref[:, span] = r
        window[n + 2] = jnp.concatenate([r, extra], axis=0).astype(jnp.bfloat16)
        return carry

    for n in (0, 1, nbr - 2, nbr - 1):
        fill(n, 0)
    halos = halo_copies(window, nbr, (end_send, end_recv), field, dom)
    start_halos(halos, dom, ends)
    copies = send_wet(
        lambda low, high: None,
        lambda cell: cell - pltpu.roll(cell, LANES - columns, 1) * across,
        spread, picked, outgoing, wet, (side_send, side_recv), (1 - field, dom),
    )
    lax.fori_loop(2, nbr - 2, fill, 0)
    blank = jnp.zeros((LANES - 3 * columns, SPAN), jnp.float32)

    def read(span):
        left = parts_of(jnp.concatenate([x_ref[:, span], p_ref[:, span], r_ref[:, span], blank], axis=0))
        split[:LANES, span] = left[0]
        split[LANES:, span] = left[1]
        right = parts_of(image[:, span])
        return left, tuple(jnp.concatenate(pair, axis=0) for pair in zip(left, right))

    gram_over(wide, read, gram)
    finish_halos(halos, dom, ends)
    for copy in copies:
        copy.wait()


def exchange_second(vec_modes, vec_prev, image, jacobi, wet_rows, wet_counts, coupling):
    columns, wide = vec_modes.shape
    slots = wet_rows.size
    rounds = sum_rounds()
    most = 2 * rounds[0][1] - 1
    return pl.pallas_call(
        functools.partial(second_kernel, rounds),
        out_shape=(
            jax.ShapeDtypeStruct((wide // BS + 5, rows_deep(columns), BS), jnp.bfloat16),
            jax.ShapeDtypeStruct((slots, LANES), jnp.bfloat16),
            jax.ShapeDtypeStruct((LANES, LANES + 2 * columns), jnp.float32),
            jax.ShapeDtypeStruct((2 * LANES, wide), jnp.bfloat16),
        ),
        in_specs=[SMEM, HBM, VMEM, VMEM, VMEM, VMEM, VMEM],
        out_specs=(VMEM,) * 4,
        scratch_shapes=exchange_scratch(wide, slots)
        + [
            pltpu.SMEM(wet_rows.shape, jnp.int32),
            pltpu.SemaphoreType.DMA((1,)),
            pltpu.VMEM((len(rounds), SUB, LANES), jnp.float32),
            pltpu.VMEM((len(rounds), most, SUB, LANES), jnp.float32),
            pltpu.SemaphoreType.DMA((len(rounds), most)),
            pltpu.SemaphoreType.DMA((len(rounds), most)),
            pltpu.VMEM((columns, wide), jnp.float32),
        ],
        compiler_params=pltpu.CompilerParams(
            collective_id=3, has_side_effects=True, vmem_limit_bytes=24 * 1024 * 1024
        ),
    )(wet_counts, wet_rows, coupling, vec_modes, vec_prev, image, jacobi)


def gram_kernel(
    rounds, split, image_r, known, o_ref,
    fresh, gram_b, gram_a, packed, held, landed, across, send_sem, recv_sem, side_send, side_recv,
):
    field = lax.axis_index("field")
    dom = lax.axis_index("dom")
    columns, wide = image_r.shape
    groups = []
    for step, members in rounds:
        low = (1 - 2 * ((dom // step) % 2)) * step
        high = (1 - 2 * ((dom // (2 * step)) % 2)) * 2 * step
        groups.append([dom + (e % 2) * low + (e // 2) * high for e in range(1, members)])
    peers = [(1 - field, dom)] + [(field, peer) for group in groups for peer in group]
    greet(peers)
    n = columns
    low = jnp.zeros((fresh.shape[0] - n, SPAN), jnp.float32)
    gram_over(
        wide,
        lambda span: (
            parts_of(jnp.concatenate([image_r[:, span], low], axis=0)),
            (split[:LANES, span], split[LANES:, span]),
        ),
        fresh,
    )
    old = known[...]
    turned = jnp.concatenate(
        [fresh[...], jnp.zeros((LANES - fresh.shape[0], LANES), jnp.float32)], axis=0
    ).T
    gram_b[...] = jnp.zeros_like(gram_b)
    gram_a[...] = jnp.zeros_like(gram_a)
    x, r, p = slice(0, n), slice(n, 2 * n), slice(2 * n, 3 * n)
    kx, kp, kr = slice(0, n), slice(n, 2 * n), slice(2 * n, 3 * n)
    ax, ap = slice(LANES, LANES + n), slice(LANES + n, LANES + 2 * n)
    for rows, here in ((x, kx), (r, kr), (p, kp)):
        gram_a[rows, x] = old[here, ax]
        gram_a[rows, r] = turned[here, :n]
        gram_a[rows, p] = old[here, ap]
    for rows, here, cols, there in (
        (x, kx, x, kx), (r, kr, x, kx), (r, kr, r, kr), (p, kp, x, kx), (p, kp, r, kr), (p, kp, p, kp),
    ):
        gram_b[rows, cols] = old[here, there]
    both = gram_a[...] + gram_a[...].T
    both = jnp.concatenate([both[:, LANES - 1 :], both[:, : LANES - 1]], axis=1)
    row = lax.broadcasted_iota(jnp.int32, (LANES, LANES), 0)
    col = lax.broadcasted_iota(jnp.int32, (LANES, LANES), 1)
    half = LANES // 2
    whole = jnp.where(col <= row, gram_b[...], both)
    packed[0] = whole[:half]
    packed[1] = whole[half:]
    pl.semaphore_wait(pltpu.get_barrier_semaphore(), len(peers))
    copy = remote(packed.at[1 - field], across.at[0], (side_send.at[0], side_recv.at[0]), (1 - field, dom))
    copy.start()
    copy.wait()
    total = packed[field] + across[0]
    for turn, group in enumerate(groups):
        held[turn] = total
        copies = [
            remote(
                held.at[turn], landed.at[turn, e], (send_sem.at[turn, e], recv_sem.at[turn, e]), (field, peer)
            )
            for e, peer in enumerate(group)
        ]
        for copy in copies:
            copy.start()
        for copy in copies:
            copy.wait()
        total = gathered(total, [landed[turn, e] for e in range(len(group))], rounds[turn][1])
    o_ref[field] = total
    held[len(groups)] = total
    copy = remote(held.at[len(groups)], across.at[1], (side_send.at[1], side_recv.at[1]), (1 - field, dom))
    copy.start()
    copy.wait()
    o_ref[1 - field] = across[1]


def gram_everywhere(split, image_r, known):
    columns = image_r.shape[0]
    rounds = sum_rounds()
    slots = len(rounds)
    cell = (LANES // 2, LANES)
    return pl.pallas_call(
        functools.partial(gram_kernel, rounds),
        out_shape=jax.ShapeDtypeStruct((2,) + cell, jnp.float32),
        in_specs=[VMEM] * 3,
        out_specs=VMEM,
        scratch_shapes=[
            pltpu.VMEM((rows_deep(columns), LANES), jnp.float32),
            pltpu.VMEM((LANES, LANES), jnp.float32),
            pltpu.VMEM((LANES, LANES), jnp.float32),
            pltpu.VMEM((2,) + cell, jnp.float32),
            pltpu.VMEM((slots + 1,) + cell, jnp.float32),
            pltpu.VMEM((slots, 3) + cell, jnp.float32),
            pltpu.VMEM((2,) + cell, jnp.float32),
            pltpu.SemaphoreType.DMA((slots, 3)),
            pltpu.SemaphoreType.DMA((slots, 3)),
            pltpu.SemaphoreType.DMA((2,)),
            pltpu.SemaphoreType.DMA((2,)),
        ],
        compiler_params=pltpu.CompilerParams(
            collective_id=2, has_side_effects=True, vmem_limit_bytes=16 * 1024 * 1024
        ),
    )(split, image_r, known)


def group_rows(kind_of, lists, nbr, types, cells, group):
    spare = nbr + 2
    bits = 32 // types
    mask = (1 << bits) - 1
    for offset in range(3):
        for slot in range(cells * group):
            lists[offset, slot] = spare
        first = 2 - offset
        shifts = [kind_of(offset, row) * bits for row in range(first, nbr + 2)]
        count = jnp.int32(0)
        ranks = []
        for shift in shifts:
            ranks.append(lax.shift_right_logical(count, shift) & mask)
            count = count + lax.shift_left(jnp.int32(1), shift)
        starts = jnp.int32(0)
        place = jnp.int32(0)
        for kind in range(types):
            starts = starts + place * (1 << bits * kind)
            here = lax.shift_right_logical(count, jnp.int32(bits * kind)) & mask
            place = place + ((here + (group - 1)) // group) * group
        for n, (shift, rank) in enumerate(zip(shifts, ranks)):
            lists[offset, (lax.shift_right_logical(starts, shift) & mask) + rank] = n + first


def operator_kernel(cells, group, with_diagonal, kinds_hbm, scales_hbm, rows_hbm, window, wet, tables, o_ref, *rest):
    if with_diagonal:
        jacobi, diagonal, total, rows_in, rows_out, lists, rows, kinds, scales, loads = rest
    else:
        total, rows_in, rows_out, lists, rows, kinds, scales, loads = rest
    columns, wide = o_ref.shape
    nbr = wide // BS
    types = tables.shape[1]
    deep = window.shape[1]
    slots = wet.shape[0]
    pairs = [(rows_hbm, rows), (kinds_hbm, kinds), (scales_hbm, scales)]
    arrivals = [pltpu.make_async_copy(source, target, loads.at[n]) for n, (source, target) in enumerate(pairs)]
    for arrival in arrivals:
        arrival.start()
    base = lax.axis_index("dom") * nbr - 2

    def kind_of(offset, row):
        return kinds[offset, 0, jnp.maximum(base + row, 0)]

    def scale_of(offset, row):
        return scales[offset, 0, jnp.maximum(base + row, 0)]

    def clear(n, carry):
        total[n] = jnp.zeros(total.shape[1:], jnp.float32)
        span = pl.ds(pl.multiple_of(n * BS, BS), BS)
        rows_out[span, :] = jnp.zeros((BS, LANES), jnp.float32)
        return carry

    lax.fori_loop(0, nbr, clear, 0)

    def widen(i, carry):
        span = pl.ds(pl.multiple_of(i * LANES, LANES), LANES)
        rows_in[span, :] = wet[span, :].astype(jnp.float32)
        return carry

    lax.fori_loop(0, slots // LANES, widen, 0, unroll=4)
    for arrival in arrivals:
        arrival.wait()

    def scatter(i, carry):
        for slot in range(LANES):
            rows_out[pl.ds(rows[i, slot], 1), :] = rows_in[pl.ds(i * LANES + slot, 1), :]
        return carry

    lax.fori_loop(0, slots // LANES, scatter, 0)
    group_rows(kind_of, lists, nbr, types, cells, group)
    if with_diagonal:
        eye = lax.broadcasted_iota(jnp.int32, (LANES, LANES), 0) == lax.broadcasted_iota(
            jnp.int32, (LANES, LANES), 1
        )
        for kind in range(types):
            for part in range(BS // LANES):
                span = slice(part * LANES, (part + 1) * LANES)
                cell = tables[0, kind, span, span].astype(jnp.float32)
                diagonal[kind, :, span] = jnp.sum(jnp.where(eye, cell, 0.0), axis=0, keepdims=True)
        for n in range(nbr):
            jacobi[:, n * BS : (n + 1) * BS] = scale_of(0, n + 2) * diagonal[kind_of(0, n + 2)]

    def step(i, carry):
        for offset in range(3):
            found = [lists[offset, i * group + u] for u in range(group)]
            held = [jnp.minimum(row, nbr + 1) for row in found]
            kind = kind_of(offset, held[0])
            factors = [scale_of(offset, row) for row in held]
            for ahead in (True, False) if offset else (True,):
                if ahead:
                    sources = [row + offset for row in found]
                    targets = [jnp.where(row < 2, nbr, row - 2) for row in found]
                else:
                    sources = found
                    targets = [jnp.minimum(row - 2 + offset, nbr) for row in found]
                left = jnp.concatenate([window[source] for source in sources], axis=0)
                product = lax.dot_general(
                    left,
                    tables[offset, kind],
                    NT if ahead and offset else NN,
                    preferred_element_type=jnp.float32,
                )
                for u in range(group):
                    total[targets[u]] += factors[u] * product[u * deep : (u + 1) * deep]
        return carry

    lax.fori_loop(0, cells, step, 0)
    parts = BS // LANES

    def turn_out(n, carry):
        for part in range(parts):
            span = pl.ds(pl.multiple_of(n * BS + part * LANES, LANES), LANES)
            inner = slice(part * LANES, (part + 1) * LANES)
            o_ref[:, span] = total[n, :columns, inner] + rows_out[span, :].T[:columns]
        return carry

    lax.fori_loop(0, nbr, turn_out, 0, unroll=4)


def operate(columns, window, wet, kinds, scales, rows, tables, with_diagonal):
    nbr = window.shape[0] - 5
    wide = nbr * BS
    deep = window.shape[1]
    slots = wet.shape[0]
    types = tables.shape[1]
    group = GROUP_WIDE if columns > LANES // 2 else GROUP
    cells = (nbr + 2 + types * (group - 1)) // group
    outs = [jax.ShapeDtypeStruct((columns, wide), jnp.float32)]
    scratch = [
        pltpu.VMEM((nbr + 1, deep, BS), jnp.float32),
        pltpu.VMEM((slots, LANES), jnp.float32),
        pltpu.VMEM((wide, LANES), jnp.float32),
        pltpu.SMEM((3, cells * group), jnp.int32),
        pltpu.SMEM(rows.shape, jnp.int32),
        pltpu.SMEM(kinds.shape, jnp.int32),
        pltpu.SMEM(scales.shape, jnp.float32),
        pltpu.SemaphoreType.DMA((3,)),
    ]
    if with_diagonal:
        outs.append(jax.ShapeDtypeStruct((1, wide), jnp.float32))
        scratch = [pltpu.VMEM((types, 1, BS), jnp.float32)] + scratch
    return pl.pallas_call(
        functools.partial(operator_kernel, cells, group, with_diagonal),
        out_shape=tuple(outs),
        in_specs=[HBM, HBM, HBM, VMEM, VMEM, VMEM],
        out_specs=(VMEM,) * len(outs),
        scratch_shapes=scratch,
        cost_estimate=pl.CostEstimate(
            flops=10 * columns * wide * BS, bytes_accessed=16 * columns * wide, transcendentals=0
        ),
        compiler_params=pltpu.CompilerParams(vmem_limit_bytes=24 * 1024 * 1024),
    )(kinds, scales, rows, window, wet, tables)


def shards(modes, previous, kinds, scales, tables, wet_rows, wet_counts, coupling):
    modes, previous, tables, wet_rows, coupling, kinds, scales = [
        pltpu.with_memory_space_constraint(array, pltpu.HBM)
        for array in (
            modes,
            previous,
            tables,
            wet_rows.reshape(-1, LANES),
            coupling.reshape(-1, LANES),
            jnp.swapaxes(kinds, 0, 1),
            jnp.swapaxes(scales, 0, 1),
        )
    ]
    _, columns, wide = modes.shape
    window, wet, vec_modes, vec_prev, field_tables, weights = exchange_first(
        modes, previous, wet_rows, wet_counts, coupling, tables
    )
    shared = (kinds, scales, wet_rows, field_tables)
    image, jacobi = operate(2 * columns, window, wet, *shared, True)
    window, wet, known, split = exchange_second(
        vec_modes, vec_prev, image, jacobi, wet_rows, wet_counts, weights
    )
    (image_r,) = operate(columns, window, wet, *shared, False)
    packed = gram_everywhere(split, image_r, known)
    ndof = 2.0 * lax.axis_size("dom") * wide
    return finish(columns, packed.reshape(LANES, LANES), split, ndof)


def solution(mesh):
    return jax.shard_map(
        shards,
        mesh=mesh,
        in_specs=(
            P("field", None, "dom"),
            P("field", None, "dom"),
            P("field", None, None),
            P("field", None, None),
            P("field", None, None, None, None),
            P("field", "dom"),
            P("dom"),
            P("dom"),
        ),
        out_specs=(P("field", None, "dom"), P()),
        check_vma=False,
    )
```

```python
import functools

import jax
import jax.numpy as jnp
from jax import lax
from jax.experimental import pallas as pl
from jax.experimental.pallas import tpu as pltpu
from jax.sharding import PartitionSpec as P

BS = 512
LANES = 128
GROUP = 5
GROUP_WIDE = 3
PARTS = 4
SPAN = 2048
MESH = pl.DeviceIdType.MESH
NN = (((1,), (0,)), ((), ()))
NT = (((1,), (1,)), ((), ()))


SUB = 8


def split_dot(left, right, dims):
    lh = left.astype(jnp.bfloat16)
    ll = (left - lh.astype(jnp.float32)).astype(jnp.bfloat16)
    rh = right.astype(jnp.bfloat16)
    rl = (right - rh.astype(jnp.float32)).astype(jnp.bfloat16)

    def dot(a, b):
        return lax.dot_general(a, b, dims, preferred_element_type=jnp.float32)

    return dot(lh, rh) + (dot(lh, rl) + dot(ll, rh))


def eliminate(gram, size, inverse_ref):
    panels = size // SUB
    sub = lax.broadcasted_iota(jnp.int32, (SUB, LANES), 0)
    lane = lax.broadcasted_iota(jnp.int32, (SUB, LANES), 1)
    left = [gram[SUB * i : SUB * (i + 1)] for i in range(panels)]
    right = [(lane == sub + SUB * i).astype(jnp.float32) for i in range(panels)]

    def over_lanes(cell, column):
        return jnp.broadcast_to(cell[:, column : column + 1], (SUB, LANES))

    def over_rows(cell, row):
        return jnp.broadcast_to(cell[row : row + 1], (SUB, LANES))

    for k in range(panels):
        columns = [over_lanes(left[k], SUB * k + c) for c in range(SUB)]
        cells = [left[k], right[k]]
        for c in range(SUB):
            pivot = over_rows(columns[c], c)
            root = lax.rsqrt(pivot)
            inverse = root * root
            inverse_ref[SUB * k + c : SUB * k + c + 1] = (cells[1] * root)[c : c + 1]
            here = sub == c
            factor = columns[c]

            def reduced(cell):
                row = over_rows(cell, c) * inverse
                return jnp.where(here, row, cell - factor * row)

            for later in range(c + 1, SUB):
                columns[later] = reduced(columns[later])
            cells = [reduced(cell) for cell in cells]
        rows = [[over_rows(cell, c) for c in range(SUB)] for cell in cells]
        for i in range(k + 1, panels):
            source = left[i]
            for c in range(SUB):
                factor = over_lanes(source, SUB * k + c)
                left[i] = left[i] - factor * rows[0][c]
                right[i] = right[i] - factor * rows[1][c]


def finish_kernel(columns, chunk, scale, packed_ref, split, basis_ref, projected_ref, inverse_ref, held, sems):
    wide = split.shape[1]
    size = 3 * columns
    packed = packed_ref[...] * scale
    row = lax.broadcasted_iota(jnp.int32, packed.shape, 0)
    col = lax.broadcasted_iota(jnp.int32, packed.shape, 1)
    gram_b = jnp.where(col <= row, packed, packed.T)
    inverse_ref[...] = jnp.zeros_like(inverse_ref)
    eliminate(gram_b, size, inverse_ref)
    high = jnp.concatenate([packed[:, 1:], packed[:, :1]], axis=1)
    gram_a = jnp.where(col >= row, high, high.T)
    gram_a = jnp.where(jnp.maximum(row, col) < size, 0.5 * gram_a, 0.0)
    inverse = inverse_ref[...]
    projected = split_dot(split_dot(inverse, gram_a, NN), inverse, NT)
    projected_ref[...] = projected[:size, :size]
    inverse = jnp.concatenate(
        [
            inverse[:, :columns],
            inverse[:, 2 * columns : size],
            inverse[:, columns : 2 * columns],
            inverse[:, size:],
        ],
        axis=1,
    )
    ih = inverse.astype(jnp.bfloat16)
    il = (inverse - ih.astype(jnp.float32)).astype(jnp.bfloat16)
    twice = jnp.concatenate([ih, ih], axis=1)

    def copy(n):
        span = pl.ds(pl.multiple_of(n * chunk, chunk), chunk)
        return pltpu.make_async_copy(held.at[n], basis_ref.at[0, :, span], sems.at[n])

    def step(n, carry):
        span = pl.ds(pl.multiple_of(n * chunk, chunk), chunk)
        out = lax.dot_general(twice, split[:, span], NN, preferred_element_type=jnp.float32)
        out = out + lax.dot_general(il, split[:LANES, span], NN, preferred_element_type=jnp.float32)
        held[n] = out[:size]
        copy(n).start()
        return carry

    lax.fori_loop(0, wide // chunk, step, 0, unroll=4)

    def close(n, carry):
        copy(n).wait()
        return carry

    lax.fori_loop(0, wide // chunk, close, 0)


def finish(columns, packed, split, ndof):
    wide = split.shape[1]
    size = 3 * columns
    chunk = min(512, wide)
    vmem = pl.BlockSpec(memory_space=pltpu.VMEM)
    return pl.pallas_call(
        functools.partial(finish_kernel, columns, chunk, 1.0 / ndof),
        out_shape=(
            jax.ShapeDtypeStruct((1, size, wide), jnp.float32),
            jax.ShapeDtypeStruct((size, size), jnp.float32),
        ),
        in_specs=[vmem, vmem],
        out_specs=(pl.BlockSpec(memory_space=pl.ANY), vmem),
        scratch_shapes=[
            pltpu.VMEM((LANES, LANES), jnp.float32),
            pltpu.VMEM((wide // chunk, size, chunk), jnp.float32),
            pltpu.SemaphoreType.DMA((wide // chunk,)),
        ],
        cost_estimate=pl.CostEstimate(
            flops=6 * size * size * wide, bytes_accessed=8 * size * wide, transcendentals=0
        ),
        compiler_params=pltpu.CompilerParams(vmem_limit_bytes=24 * 1024 * 1024),
    )(packed, split)


def remote(source, target, sems, peer):
    return pltpu.make_async_remote_copy(
        src_ref=source,
        dst_ref=target,
        send_sem=sems[0],
        recv_sem=sems[1],
        device_id=peer,
        device_id_type=MESH,
    )


def greet(peers):
    barrier = pltpu.get_barrier_semaphore()
    for peer in peers:
        pl.semaphore_signal(barrier, inc=1, device_id=peer, device_id_type=MESH)


def greet_ends(field, dom, ends):
    barrier = pltpu.get_barrier_semaphore()

    @pl.when(dom > 0)
    def _():
        pl.semaphore_signal(barrier, inc=1, device_id=(field, dom - 1), device_id_type=MESH)

    @pl.when(dom < ends)
    def _():
        pl.semaphore_signal(barrier, inc=1, device_id=(field, dom + 1), device_id_type=MESH)


def meet(dom, ends, count):
    left = (dom + ends - 1) // ends
    right = (2 * ends - dom - 1) // ends
    pl.semaphore_wait(pltpu.get_barrier_semaphore(), count + left + right)


def clear_ends(window, nbr):
    empty = jnp.zeros((2,) + window.shape[1:], window.dtype)
    window[:2] = empty
    window[nbr + 2 : nbr + 4] = empty


def halo_copies(window, nbr, sems, field, dom):
    send, recv = sems
    left = remote(
        window.at[pl.ds(2, 2)], window.at[pl.ds(nbr + 2, 2)], (send.at[0], recv.at[0]), (field, dom - 1)
    )
    right = remote(
        window.at[pl.ds(nbr, 2)], window.at[pl.ds(0, 2)], (send.at[1], recv.at[1]), (field, dom + 1)
    )
    return left, right


def start_halos(copies, dom, ends):
    left, right = copies

    @pl.when(dom > 0)
    def _():
        left.start()

    @pl.when(dom < ends)
    def _():
        right.start()


def finish_halos(copies, dom, ends):
    left, right = copies

    @pl.when(dom > 0)
    def _():
        left.wait_send()
        right.wait_recv()

    @pl.when(dom < ends)
    def _():
        right.wait_send()
        left.wait_recv()


def turn_rows(read, columns, wide, rows_in):
    blank = jnp.zeros((LANES - columns, LANES), jnp.float32)

    def turn_in(tile, carry):
        span = pl.ds(pl.multiple_of(tile * LANES, LANES), LANES)
        rows_in[span, :] = jnp.concatenate([read(span), blank], axis=0).T
        return carry

    lax.fori_loop(0, wide // LANES, turn_in, 0, unroll=16)


def pick_rows(low, high, rows, rows_in, picked):
    def gather(i, carry):
        for slot in range(LANES):
            picked[pl.ds(i * LANES + slot, 1), :] = rows_in[pl.ds(rows[i, slot], 1), :]
        return carry

    lax.fori_loop(low, high, gather, 0)


def spread_weights(count, coupling, spread):
    def one(i, carry):
        span = pl.ds(pl.multiple_of(i * LANES, LANES), LANES)
        used = i * LANES + lax.broadcasted_iota(jnp.int32, (1, LANES), 1) < count
        weights = jnp.where(used, coupling[pl.ds(i, 1), :], 0.0)
        spread[span, :] = jnp.broadcast_to(weights, (LANES, LANES)).T
        return carry

    lax.fori_loop(0, coupling.shape[0], one, 0, unroll=4)


def send_wet(prepare, combine, spread, picked, outgoing, wet, sems, peer):
    cells = picked.shape[0] // LANES

    def weigh(i, carry):
        span = pl.ds(pl.multiple_of(i * LANES, LANES), LANES)
        outgoing[span, :] = (combine(picked[span, :]) * spread[span, :]).astype(jnp.bfloat16)
        return carry

    copies = []
    for part in range(PARTS):
        low, high = cells * part // PARTS, cells * (part + 1) // PARTS
        prepare(low, high)
        lax.fori_loop(low, high, weigh, 0, unroll=2)
        span = pl.ds(low * LANES, (high - low) * LANES)
        copy = remote(outgoing.at[span], wet.at[span], (sems[0].at[part], sems[1].at[part]), peer)
        copy.start()
        copies.append(copy)
    return copies


def first_kernel(
    counts, rows_in_hbm, coupling_in, x_in, p_in, tables_in, kinds_in, scales_in,
    window, wet, x_ref, p_ref, tables, coupling, rows_out, kinds_out, scales_out,
    rows_in, picked, spread, outgoing, side_send, side_recv, end_send, end_recv, rows, loads,
):
    field = lax.axis_index("field")
    dom = lax.axis_index("dom")
    ends = lax.axis_size("dom") - 1
    columns, wide = x_ref.shape
    nbr = wide // BS
    pairs = [(x_in.at[0], x_ref), (p_in.at[0], p_ref), (rows_in_hbm, rows), (coupling_in, coupling), (tables_in.at[0], tables)]
    pairs += [(rows_in_hbm, rows_out), (kinds_in, kinds_out), (scales_in, scales_out)]
    arrivals = [pltpu.make_async_copy(source, target, loads.at[n]) for n, (source, target) in enumerate(pairs)]
    for arrival in arrivals[:4]:
        arrival.start()
    clear_ends(window, nbr)
    greet([(1 - field, dom)])
    greet_ends(field, dom, ends)

    def read(span):
        return jnp.concatenate([x_ref[:, span], p_ref[:, span]], axis=0)

    def fill(n, carry):
        span = pl.ds(pl.multiple_of(n * BS, BS), BS)
        window[n + 2] = read(span).astype(jnp.bfloat16)
        return carry

    arrivals[3].wait()
    spread_weights(counts[0], coupling, spread)
    arrivals[0].wait()
    arrivals[1].wait()
    for arrival in arrivals[4:]:
        arrival.start()
    lax.fori_loop(0, nbr, fill, 0, unroll=2)
    meet(dom, ends, 1)
    halos = halo_copies(window, nbr, (end_send, end_recv), field, dom)
    start_halos(halos, dom, ends)
    arrivals[2].wait()
    turn_rows(read, 2 * columns, wide, rows_in)
    copies = send_wet(
        lambda low, high: pick_rows(low, high, rows, rows_in, picked),
        lambda cell: cell, spread, picked, outgoing, wet, (side_send, side_recv), (1 - field, dom),
    )
    for arrival in arrivals[4:]:
        arrival.wait()
    finish_halos(halos, dom, ends)
    for copy in copies:
        copy.wait()


def exchange_scratch(wide, slots):
    return [
        pltpu.VMEM((wide, LANES), jnp.float32),
        pltpu.VMEM((slots, LANES), jnp.float32),
        pltpu.VMEM((slots, LANES), jnp.float32),
        pltpu.VMEM((slots, LANES), jnp.bfloat16),
        pltpu.SemaphoreType.DMA((PARTS,)),
        pltpu.SemaphoreType.DMA((PARTS,)),
        pltpu.SemaphoreType.DMA((2,)),
        pltpu.SemaphoreType.DMA((2,)),
    ]


def rows_deep(columns):
    return -(-columns // 16) * 16


SMEM = pl.BlockSpec(memory_space=pltpu.SMEM)
VMEM = pl.BlockSpec(memory_space=pltpu.VMEM)
HBM = pl.BlockSpec(memory_space=pltpu.HBM)


def exchange_first(modes, previous, wet_rows, wet_counts, coupling, tables, kinds, scales):
    _, columns, wide = modes.shape
    slots = wet_rows.size
    held = jax.ShapeDtypeStruct((columns, wide), jnp.float32)
    return pl.pallas_call(
        first_kernel,
        out_shape=(
            jax.ShapeDtypeStruct((wide // BS + 5, rows_deep(2 * columns), BS), jnp.bfloat16),
            jax.ShapeDtypeStruct((slots, LANES), jnp.bfloat16),
            held,
            held,
            jax.ShapeDtypeStruct(tables.shape[1:], tables.dtype),
            jax.ShapeDtypeStruct(coupling.shape, coupling.dtype),
            jax.ShapeDtypeStruct(wet_rows.shape, wet_rows.dtype),
            jax.ShapeDtypeStruct(kinds.shape, kinds.dtype),
            jax.ShapeDtypeStruct(scales.shape, scales.dtype),
        ),
        in_specs=[SMEM] + [HBM] * 7,
        out_specs=(VMEM,) * 9,
        scratch_shapes=exchange_scratch(wide, slots)
        + [pltpu.SMEM(wet_rows.shape, jnp.int32), pltpu.SemaphoreType.DMA((8,))],
        compiler_params=pltpu.CompilerParams(
            collective_id=1, has_side_effects=True, vmem_limit_bytes=24 * 1024 * 1024
        ),
    )(wet_counts, wet_rows, coupling, modes, previous, tables, kinds, scales)


def parts_of(cell):
    high = cell.astype(jnp.bfloat16)
    return high, (cell - high.astype(jnp.float32)).astype(jnp.bfloat16)


def gram_over(wide, read, out):
    out[...] = jnp.zeros_like(out)
    count = out.shape[0]

    def add(n, carry):
        span = pl.ds(pl.multiple_of(n * SPAN, SPAN), SPAN)
        (lh, ll), (rh, rl) = read(span)
        both = lax.dot_general(
            jnp.concatenate([lh, ll], axis=0), rh, NT, preferred_element_type=jnp.float32
        )
        cross = lax.dot_general(lh, rl, NT, preferred_element_type=jnp.float32)
        out[...] += both[:count] + (both[count:] + cross)
        return carry

    lax.fori_loop(0, wide // SPAN, add, 0)


def neighbours(rounds, field, dom):
    groups = []
    for turn, (step, members) in enumerate(rounds):
        low = (1 - 2 * ((dom // step) % 2)) * step
        high = (1 - 2 * ((dom // (2 * step)) % 2)) * 2 * step
        group = [(field, dom + (e % 2) * low + (e // 2) * high) for e in range(members)]
        across = [(1 - field, there) for _, there in group] if turn == 0 else []
        groups.append(group[1:] + across)
    return groups


def gathered(total, landed, members):
    def fold(parts):
        if len(parts) == 4:
            return (parts[0] + parts[1]) + (parts[2] + parts[3])
        return parts[0] + parts[1]

    parts = [total] + landed
    total = fold(parts[:members])
    return total + fold(parts[members:]) if len(parts) > members else total


def sum_rounds():
    bits = (lax.axis_size("dom") - 1).bit_length()
    return [(1 << bit, 4 if bit + 1 < bits else 2) for bit in range(0, bits, 2)]


def second_kernel(
    rounds, counts, rows_hbm, coupling, x_ref, p_ref, image, jacobi, window, wet, gram, split,
    rows_in, picked, spread, outgoing, side_send, side_recv, end_send, end_recv,
    rows, loads, held, landed, sum_send, sum_recv, r_ref,
):
    field = lax.axis_index("field")
    dom = lax.axis_index("dom")
    ends = lax.axis_size("dom") - 1
    columns, wide = x_ref.shape
    nbr = wide // BS
    deep = window.shape[1]
    arrival = pltpu.make_async_copy(rows_hbm, rows, loads.at[0])
    arrival.start()
    groups = neighbours(rounds, field, dom)
    clear_ends(window, nbr)
    peers = [peer for group in groups for peer in group]
    greet(peers)
    greet_ends(field, dom, ends)

    def add(n, carry):
        span = pl.ds(pl.multiple_of(n * LANES, LANES), LANES)
        x = x_ref[:, span]
        return carry[0] + x * x, carry[1] + x * image[:columns, span]

    zero = jnp.zeros((columns, LANES), jnp.float32)
    squares, products = lax.fori_loop(0, wide // LANES, add, (zero, zero), unroll=8)
    lane = lax.broadcasted_iota(jnp.int32, (columns, LANES), 1)
    total = jnp.where(
        lane == 0,
        jnp.sum(squares, axis=1, keepdims=True),
        jnp.where(lane == 1, jnp.sum(products, axis=1, keepdims=True), 0.0),
    )
    total = jnp.concatenate([total, jnp.zeros((LANES - columns, LANES), jnp.float32)], axis=0).T[:SUB]
    arrival.wait()
    meet(dom, ends, len(peers))
    for turn, group in enumerate(groups):
        held[turn] = total
        copies = [
            remote(held.at[turn], landed.at[turn, e], (sum_send.at[turn, e], sum_recv.at[turn, e]), peer)
            for e, peer in enumerate(group)
        ]
        for copy in copies:
            copy.start()
        if turn == 0:
            turn_rows(
                lambda span: jnp.concatenate(
                    [image[:columns, span] / jacobi[:, span], x_ref[:, span] / jacobi[:, span]], axis=0
                ),
                2 * columns, wide, rows_in,
            )
        if turn == len(groups) - 1:
            pick_rows(0, rows.shape[0], rows, rows_in, picked)
            spread_weights(counts[0], coupling, spread)
        for copy in copies:
            copy.wait()
        members = rounds[turn][1]
        total = gathered(total, [landed[turn, e] for e in range(len(group))], members)
    lane = lax.broadcasted_iota(jnp.int32, (1, LANES), 1)
    across = jnp.where(lane < columns, total[1:2] / total[0:1], 0.0)
    total = jnp.concatenate([total, jnp.zeros((LANES - SUB, LANES), jnp.float32)], axis=0).T[:columns]
    quotient = total[:, 1:2] / total[:, 0:1]
    extra = jnp.zeros((deep - columns, BS), jnp.float32)

    def fill(n, carry):
        span = pl.ds(pl.multiple_of(n * BS, BS), BS)
        r = (image[:columns, span] - x_ref[:, span] * quotient) / jacobi[:, span]
        r_ref[:, span] = r
        window[n + 2] = jnp.concatenate([r, extra], axis=0).astype(jnp.bfloat16)
        return carry

    for n in (0, 1, nbr - 2, nbr - 1):
        fill(n, 0)
    halos = halo_copies(window, nbr, (end_send, end_recv), field, dom)
    start_halos(halos, dom, ends)
    copies = send_wet(
        lambda low, high: None,
        lambda cell: cell - pltpu.roll(cell, LANES - columns, 1) * across,
        spread, picked, outgoing, wet, (side_send, side_recv), (1 - field, dom),
    )
    lax.fori_loop(2, nbr - 2, fill, 0)
    blank = jnp.zeros((LANES - 3 * columns, SPAN), jnp.float32)

    def read(span):
        left = parts_of(jnp.concatenate([x_ref[:, span], p_ref[:, span], r_ref[:, span], blank], axis=0))
        split[:LANES, span] = left[0]
        split[LANES:, span] = left[1]
        right = parts_of(image[:, span])
        return left, tuple(jnp.concatenate(pair, axis=0) for pair in zip(left, right))

    gram_over(wide, read, gram)
    finish_halos(halos, dom, ends)
    for copy in copies:
        copy.wait()


def exchange_second(vec_modes, vec_prev, image, jacobi, wet_rows, wet_counts, coupling):
    columns, wide = vec_modes.shape
    slots = wet_rows.size
    rounds = sum_rounds()
    most = 2 * rounds[0][1] - 1
    return pl.pallas_call(
        functools.partial(second_kernel, rounds),
        out_shape=(
            jax.ShapeDtypeStruct((wide // BS + 5, rows_deep(columns), BS), jnp.bfloat16),
            jax.ShapeDtypeStruct((slots, LANES), jnp.bfloat16),
            jax.ShapeDtypeStruct((LANES, LANES + 2 * columns), jnp.float32),
            jax.ShapeDtypeStruct((2 * LANES, wide), jnp.bfloat16),
        ),
        in_specs=[SMEM, VMEM, VMEM, VMEM, VMEM, VMEM, VMEM],
        out_specs=(VMEM,) * 4,
        scratch_shapes=exchange_scratch(wide, slots)
        + [
            pltpu.SMEM(wet_rows.shape, jnp.int32),
            pltpu.SemaphoreType.DMA((1,)),
            pltpu.VMEM((len(rounds), SUB, LANES), jnp.float32),
            pltpu.VMEM((len(rounds), most, SUB, LANES), jnp.float32),
            pltpu.SemaphoreType.DMA((len(rounds), most)),
            pltpu.SemaphoreType.DMA((len(rounds), most)),
            pltpu.VMEM((columns, wide), jnp.float32),
        ],
        compiler_params=pltpu.CompilerParams(
            collective_id=3, has_side_effects=True, vmem_limit_bytes=24 * 1024 * 1024
        ),
    )(wet_counts, wet_rows, coupling, vec_modes, vec_prev, image, jacobi)


def gram_kernel(
    rounds, split, image_r, known, o_ref,
    fresh, gram_b, gram_a, packed, held, landed, across, send_sem, recv_sem, side_send, side_recv,
):
    field = lax.axis_index("field")
    dom = lax.axis_index("dom")
    columns, wide = image_r.shape
    groups = []
    for step, members in rounds:
        low = (1 - 2 * ((dom // step) % 2)) * step
        high = (1 - 2 * ((dom // (2 * step)) % 2)) * 2 * step
        groups.append([dom + (e % 2) * low + (e // 2) * high for e in range(1, members)])
    peers = [(1 - field, dom)] + [(field, peer) for group in groups for peer in group]
    greet(peers)
    n = columns
    low = jnp.zeros((fresh.shape[0] - n, SPAN), jnp.float32)
    gram_over(
        wide,
        lambda span: (
            parts_of(jnp.concatenate([image_r[:, span], low], axis=0)),
            (split[:LANES, span], split[LANES:, span]),
        ),
        fresh,
    )
    old = known[...]
    turned = jnp.concatenate(
        [fresh[...], jnp.zeros((LANES - fresh.shape[0], LANES), jnp.float32)], axis=0
    ).T
    gram_b[...] = jnp.zeros_like(gram_b)
    gram_a[...] = jnp.zeros_like(gram_a)
    x, r, p = slice(0, n), slice(n, 2 * n), slice(2 * n, 3 * n)
    kx, kp, kr = slice(0, n), slice(n, 2 * n), slice(2 * n, 3 * n)
    ax, ap = slice(LANES, LANES + n), slice(LANES + n, LANES + 2 * n)
    for rows, here in ((x, kx), (r, kr), (p, kp)):
        gram_a[rows, x] = old[here, ax]
        gram_a[rows, r] = turned[here, :n]
        gram_a[rows, p] = old[here, ap]
    for rows, here, cols, there in (
        (x, kx, x, kx), (r, kr, x, kx), (r, kr, r, kr), (p, kp, x, kx), (p, kp, r, kr), (p, kp, p, kp),
    ):
        gram_b[rows, cols] = old[here, there]
    both = gram_a[...] + gram_a[...].T
    both = jnp.concatenate([both[:, LANES - 1 :], both[:, : LANES - 1]], axis=1)
    row = lax.broadcasted_iota(jnp.int32, (LANES, LANES), 0)
    col = lax.broadcasted_iota(jnp.int32, (LANES, LANES), 1)
    half = LANES // 2
    whole = jnp.where(col <= row, gram_b[...], both)
    packed[0] = whole[:half]
    packed[1] = whole[half:]
    pl.semaphore_wait(pltpu.get_barrier_semaphore(), len(peers))
    copy = remote(packed.at[1 - field], across.at[0], (side_send.at[0], side_recv.at[0]), (1 - field, dom))
    copy.start()
    copy.wait()
    total = packed[field] + across[0]
    for turn, group in enumerate(groups):
        held[turn] = total
        copies = [
            remote(
                held.at[turn], landed.at[turn, e], (send_sem.at[turn, e], recv_sem.at[turn, e]), (field, peer)
            )
            for e, peer in enumerate(group)
        ]
        for copy in copies:
            copy.start()
        for copy in copies:
            copy.wait()
        total = gathered(total, [landed[turn, e] for e in range(len(group))], rounds[turn][1])
    o_ref[field] = total
    held[len(groups)] = total
    copy = remote(held.at[len(groups)], across.at[1], (side_send.at[1], side_recv.at[1]), (1 - field, dom))
    copy.start()
    copy.wait()
    o_ref[1 - field] = across[1]


def gram_everywhere(split, image_r, known):
    columns = image_r.shape[0]
    rounds = sum_rounds()
    slots = len(rounds)
    cell = (LANES // 2, LANES)
    return pl.pallas_call(
        functools.partial(gram_kernel, rounds),
        out_shape=jax.ShapeDtypeStruct((2,) + cell, jnp.float32),
        in_specs=[VMEM] * 3,
        out_specs=VMEM,
        scratch_shapes=[
            pltpu.VMEM((rows_deep(columns), LANES), jnp.float32),
            pltpu.VMEM((LANES, LANES), jnp.float32),
            pltpu.VMEM((LANES, LANES), jnp.float32),
            pltpu.VMEM((2,) + cell, jnp.float32),
            pltpu.VMEM((slots + 1,) + cell, jnp.float32),
            pltpu.VMEM((slots, 3) + cell, jnp.float32),
            pltpu.VMEM((2,) + cell, jnp.float32),
            pltpu.SemaphoreType.DMA((slots, 3)),
            pltpu.SemaphoreType.DMA((slots, 3)),
            pltpu.SemaphoreType.DMA((2,)),
            pltpu.SemaphoreType.DMA((2,)),
        ],
        compiler_params=pltpu.CompilerParams(
            collective_id=2, has_side_effects=True, vmem_limit_bytes=16 * 1024 * 1024
        ),
    )(split, image_r, known)


def group_rows(kind_of, lists, nbr, types, cells, group):
    spare = nbr + 2
    bits = 32 // types
    mask = (1 << bits) - 1
    for offset in range(3):
        for slot in range(cells * group):
            lists[offset, slot] = spare
        first = 2 - offset
        shifts = [kind_of(offset, row) * bits for row in range(first, nbr + 2)]
        count = jnp.int32(0)
        ranks = []
        for shift in shifts:
            ranks.append(lax.shift_right_logical(count, shift) & mask)
            count = count + lax.shift_left(jnp.int32(1), shift)
        starts = jnp.int32(0)
        place = jnp.int32(0)
        for kind in range(types):
            starts = starts + place * (1 << bits * kind)
            here = lax.shift_right_logical(count, jnp.int32(bits * kind)) & mask
            place = place + ((here + (group - 1)) // group) * group
        for n, (shift, rank) in enumerate(zip(shifts, ranks)):
            lists[offset, (lax.shift_right_logical(starts, shift) & mask) + rank] = n + first


def operator_kernel(cells, group, with_diagonal, kinds_hbm, scales_hbm, rows_hbm, window, wet, tables, o_ref, *rest):
    if with_diagonal:
        jacobi, diagonal, total, rows_in, rows_out, lists, rows, kinds, scales, loads = rest
    else:
        total, rows_in, rows_out, lists, rows, kinds, scales, loads = rest
    columns, wide = o_ref.shape
    nbr = wide // BS
    types = tables.shape[1]
    deep = window.shape[1]
    slots = wet.shape[0]
    pairs = [(rows_hbm, rows), (kinds_hbm, kinds), (scales_hbm, scales)]
    arrivals = [pltpu.make_async_copy(source, target, loads.at[n]) for n, (source, target) in enumerate(pairs)]
    for arrival in arrivals:
        arrival.start()
    base = lax.axis_index("dom") * nbr - 2

    def kind_of(offset, row):
        return kinds[offset, 0, jnp.maximum(base + row, 0)]

    def scale_of(offset, row):
        return scales[offset, 0, jnp.maximum(base + row, 0)]

    def clear(n, carry):
        total[n] = jnp.zeros(total.shape[1:], jnp.float32)
        span = pl.ds(pl.multiple_of(n * BS, BS), BS)
        rows_out[span, :] = jnp.zeros((BS, LANES), jnp.float32)
        return carry

    lax.fori_loop(0, nbr, clear, 0)

    def widen(i, carry):
        span = pl.ds(pl.multiple_of(i * LANES, LANES), LANES)
        rows_in[span, :] = wet[span, :].astype(jnp.float32)
        return carry

    lax.fori_loop(0, slots // LANES, widen, 0, unroll=4)
    for arrival in arrivals:
        arrival.wait()

    for i in range(slots // LANES):
        for slot in range(LANES):
            at = i * LANES + slot
            rows_out[pl.ds(rows[i, slot], 1), :] = rows_in[at : at + 1, :]
    group_rows(kind_of, lists, nbr, types, cells, group)
    if with_diagonal:
        eye = lax.broadcasted_iota(jnp.int32, (LANES, LANES), 0) == lax.broadcasted_iota(
            jnp.int32, (LANES, LANES), 1
        )
        for kind in range(types):
            for part in range(BS // LANES):
                span = slice(part * LANES, (part + 1) * LANES)
                cell = tables[0, kind, span, span].astype(jnp.float32)
                diagonal[kind, :, span] = jnp.sum(jnp.where(eye, cell, 0.0), axis=0, keepdims=True)
        for n in range(nbr):
            jacobi[:, n * BS : (n + 1) * BS] = scale_of(0, n + 2) * diagonal[kind_of(0, n + 2)]

    tiles = wide // LANES
    share = -(-tiles // cells)

    def step(i, carry):
        for part in range(share):
            tile = jnp.minimum(i * share + part, tiles - 1)
            span = pl.ds(pl.multiple_of(tile * LANES, LANES), LANES)
            o_ref[:, span] = rows_out[span, :].T[:columns]
        for offset in range(3):
            found = [lists[offset, i * group + u] for u in range(group)]
            held = [jnp.minimum(row, nbr + 1) for row in found]
            kind = kind_of(offset, held[0])
            factors = [scale_of(offset, row) for row in held]
            for ahead in (True, False) if offset else (True,):
                if ahead:
                    sources = [row + offset for row in found]
                    targets = [jnp.where(row < 2, nbr, row - 2) for row in found]
                else:
                    sources = found
                    targets = [jnp.minimum(row - 2 + offset, nbr) for row in found]
                left = jnp.concatenate([window[source] for source in sources], axis=0)
                product = lax.dot_general(
                    left,
                    tables[offset, kind],
                    NT if ahead and offset else NN,
                    preferred_element_type=jnp.float32,
                )
                for u in range(group):
                    total[targets[u]] += factors[u] * product[u * deep : (u + 1) * deep]
        return carry

    lax.fori_loop(0, cells, step, 0, unroll=2)

    def close(n, carry):
        span = pl.ds(pl.multiple_of(n * BS, BS), BS)
        o_ref[:, span] = o_ref[:, span] + total[n, :columns]
        return carry

    lax.fori_loop(0, nbr, close, 0, unroll=2)


def operate(columns, window, wet, kinds, scales, rows, tables, with_diagonal):
    nbr = window.shape[0] - 5
    wide = nbr * BS
    deep = window.shape[1]
    slots = wet.shape[0]
    types = tables.shape[1]
    group = GROUP_WIDE if columns > LANES // 2 else GROUP
    cells = (nbr + 2 + types * (group - 1)) // group
    outs = [jax.ShapeDtypeStruct((columns, wide), jnp.float32)]
    scratch = [
        pltpu.VMEM((nbr + 1, deep, BS), jnp.float32),
        pltpu.VMEM((slots, LANES), jnp.float32),
        pltpu.VMEM((wide, LANES), jnp.float32),
        pltpu.SMEM((3, cells * group), jnp.int32),
        pltpu.SMEM(rows.shape, jnp.int32),
        pltpu.SMEM(kinds.shape, jnp.int32),
        pltpu.SMEM(scales.shape, jnp.float32),
        pltpu.SemaphoreType.DMA((3,)),
    ]
    if with_diagonal:
        outs.append(jax.ShapeDtypeStruct((1, wide), jnp.float32))
        scratch = [pltpu.VMEM((types, 1, BS), jnp.float32)] + scratch
    return pl.pallas_call(
        functools.partial(operator_kernel, cells, group, with_diagonal),
        out_shape=tuple(outs),
        in_specs=[VMEM] * 6,
        out_specs=(VMEM,) * len(outs),
        scratch_shapes=scratch,
        cost_estimate=pl.CostEstimate(
            flops=10 * columns * wide * BS, bytes_accessed=16 * columns * wide, transcendentals=0
        ),
        compiler_params=pltpu.CompilerParams(vmem_limit_bytes=24 * 1024 * 1024),
    )(kinds, scales, rows, window, wet, tables)


def shards(modes, previous, kinds, scales, tables, wet_rows, wet_counts, coupling):
    modes, previous, tables, wet_rows, coupling, kinds, scales = [
        pltpu.with_memory_space_constraint(array, pltpu.HBM)
        for array in (
            modes,
            previous,
            tables,
            wet_rows.reshape(-1, LANES),
            coupling.reshape(-1, LANES),
            jnp.swapaxes(kinds, 0, 1),
            jnp.swapaxes(scales, 0, 1),
        )
    ]
    _, columns, wide = modes.shape
    window, wet, vec_modes, vec_prev, field_tables, weights, wet_rows, kinds, scales = exchange_first(
        modes, previous, wet_rows, wet_counts, coupling, tables, kinds, scales
    )
    shared = (kinds, scales, wet_rows, field_tables)
    image, jacobi = operate(2 * columns, window, wet, *shared, True)
    window, wet, known, split = exchange_second(
        vec_modes, vec_prev, image, jacobi, wet_rows, wet_counts, weights
    )
    (image_r,) = operate(columns, window, wet, *shared, False)
    packed = gram_everywhere(split, image_r, known)
    ndof = 2.0 * lax.axis_size("dom") * wide
    return finish(columns, packed.reshape(LANES, LANES), split, ndof)


def solution(mesh):
    return jax.shard_map(
        shards,
        mesh=mesh,
        in_specs=(
            P("field", None, "dom"),
            P("field", None, "dom"),
            P("field", None, None),
            P("field", None, None),
            P("field", None, None, None, None),
            P("field", "dom"),
            P("dom"),
            P("dom"),
        ),
        out_specs=(P("field", None, "dom"), P()),
        check_vma=False,
    )
```
